256 devices in a mesh: fsdp: 8 (over x, core), vocab: 32 (over y, z).
Axes of the slice: x: 4, y: 4, z: 8, core: 2. Of those that a mesh axis runs over, the one named last changes fastest.
Arguments:
- hidden_states: bfloat16 [1024, 3072], P('fsdp', 'vocab'), may hold values from -512 to 512
- head: bfloat16 [3072, 65536], P('fsdp', 'vocab'), may hold values from -0.25259074 to 0.25259074
- labels: int32 [1024], P('fsdp'), may hold values from 0 to 65535
Outputs:
- token_loss: float32 [1024], P('fsdp')
- state_grad: bfloat16 [1024, 3072], P('fsdp', 'vocab')
- head_grad: float32 [3072, 65536], P('fsdp', 'vocab')
The draws below stay inside these ranges and needn't reach their ends.
All inputs are finite; a program needn't handle non-finite values.
Results may differ from the reference program's by a relative error of at most 0.0034.
Values may be sent and summed in bfloat16 or wider, within the bound.
No kernel may reach another device: no remote copies, remote signals or barrier semaphores. Data moves between devices by JAX's collectives and lax.ppermute only.
A program may use at most 128 MiB of HBM per device.

```python
import math
import jax
import jax.numpy as jnp
from jax import lax

D = 3072
TOK_DEV = 128
VOCAB = 65536
TOKENS = 1024


def head_matrix(key):
    base = jax.random.fold_in(key, 11)
    noise_key, spread_key = jax.random.split(base)
    noise = jnp.clip(jax.random.normal(noise_key, (D, VOCAB), jnp.float32), -5.0, 5.0)
    spread = jnp.exp(jax.random.uniform(spread_key, (VOCAB,), jnp.float32, math.log(0.8), math.log(1.25)))
    ramp = jnp.exp(math.log(2.2) * jnp.arange(VOCAB, dtype=jnp.float32) / VOCAB)
    return noise * (spread * ramp)[None, :] / math.sqrt(D)


def draw_head(key, part):
    return head_matrix(key).astype(jnp.bfloat16)


def draw_hidden_states(key, part):
    base = jax.random.fold_in(key, 23)
    scale_key, value_key = jax.random.split(base, 2)
    scale = jnp.exp(jax.random.uniform(scale_key, (TOKENS, 1), jnp.float32, math.log(0.35), math.log(1.0)))
    values = jnp.clip(jax.random.normal(value_key, (TOKENS, D), jnp.float32), -5.0, 5.0) * scale
    return values.astype(jnp.bfloat16)


def set_ends(array, rng, least, high):
    place = [jax.random.randint(jax.random.fold_in(rng, axis), (), 0, length) for axis, length in enumerate(array.shape)]
    longest = array.shape.index(max(array.shape))
    neighbour = place[:longest] + [(place[longest] + 1) % array.shape[longest]] + place[longest + 1:]
    return array.at[tuple(place)].set(least).at[tuple(neighbour)].set(high)


def setup_inputs(seed: int = 0) -> dict:
    splits = jax.random.split(jax.random.key(seed), 4)
    return {
        "hidden_states": draw_hidden_states(jax.random.fold_in(splits[3], 71), 0),
        "head": draw_head(jax.random.fold_in(splits[3], 71), 0),
        "labels": set_ends(jax.random.randint(splits[2], (TOKENS,), 0, VOCAB), jax.random.fold_in(splits[2], 1), 0, VOCAB - 1).astype(jnp.int32),
    }


def reference(hidden_states, head, labels):
    groups = TOKENS // TOK_DEV
    states = hidden_states.reshape(groups, TOK_DEV, D)
    targets = labels.reshape(groups, TOK_DEV)
    columns = jnp.arange(VOCAB, dtype=jnp.int32)

    def one_group(grad_sum, pair):
        block, wanted = pair
        logits = jnp.dot(block, head, preferred_element_type=jnp.float32)
        peak = jnp.max(logits, axis=1)
        shifted = jnp.exp(logits - peak[:, None])
        total = jnp.sum(shifted, axis=1)
        hits = wanted[:, None] == columns[None, :]
        target = jnp.sum(jnp.where(hits, logits, jnp.float32(0.0)), axis=1)
        loss = jnp.log(total) + peak - target
        errors = (shifted / total[:, None] - hits.astype(jnp.float32)).astype(jnp.bfloat16)
        state_part = lax.dot_general(errors, head, (((1,), (1,)), ((), ())), preferred_element_type=jnp.float32)
        term = lax.dot_general(block, errors, (((0,), (0,)), ((), ())), preferred_element_type=jnp.float32)
        return grad_sum + term, (loss, state_part.astype(jnp.bfloat16))

    start = jnp.zeros((D, VOCAB), jnp.float32)
    head_grad, outputs = lax.scan(one_group, start, (states, targets))
    token_loss = outputs[0].reshape(TOKENS)
    state_grad = outputs[1].reshape(TOKENS, D)
    return (token_loss, state_grad, head_grad)
```

```python
import jax
import jax.numpy as jnp
from jax import lax
from jax.sharding import Mesh, PartitionSpec as P


BF = jnp.bfloat16
F32 = jnp.float32
NX, NY, NZ = 4, 4, 8


def shift(a, axis, n, s):
    return lax.ppermute(a, axis, [(i, (i + s) % n) for i in range(n)])


def swap(a):
    return lax.ppermute(a, "core", [(0, 1), (1, 0)])


def ordered(parts, index):
    n = len(parts)
    both = jnp.stack(parts + parts[:-1])
    return lax.dynamic_slice_in_dim(both, (n - index) % n, n, 0)


def gathered(a, axis, n):
    parts = [a] + [shift(a, axis, n, -j) for j in range(1, n)]
    return ordered(parts, lax.axis_index(axis))


def combined(parts):
    peaks = parts[:, 0]
    peak = jnp.max(peaks, axis=0)
    total = jnp.sum(parts[:, 1] * jnp.exp(peaks - peak), axis=0)
    return jnp.stack([peak, total, jnp.sum(parts[:, 2], axis=0)])


def local(hidden_states, head, labels):
    x, core, y = lax.axis_index("x"), lax.axis_index("core"), lax.axis_index("y")
    vocab = y * NZ + lax.axis_index("z")
    tokens, part = hidden_states.shape
    rows, width = head.shape
    half = rows // 2

    mine = hidden_states.T
    spread = jnp.broadcast_to(mine[None], (NY * NZ, part, tokens))
    features = lax.all_to_all(spread, ("y", "z"), 0, 0, tiled=True)
    flat = features.reshape(NY * NZ * part, tokens)

    low, high = head[:half], head[half:]
    up_low = shift(low, "x", NX, 1)
    down_high = shift(high, "x", NX, -1)
    up_high = shift(high, "x", NX, 1)
    down_low = shift(low, "x", NX, -1)
    far_low = shift(up_low, "x", NX, 1)
    far_high = shift(down_high, "x", NX, -1)
    held = [
        (head, 0, 0),
        (up_low, 3, 0),
        (down_high, 1, half),
        (up_high, 3, half),
        (down_low, 1, 0),
        (far_low, 2, 0),
        (far_high, 2, half),
    ]
    chunks = []
    for array, offset, first in held:
        base = ((x + offset) % NX) * 2
        chunks.append((array, (base + core) * rows + first))
        chunks.append((swap(array), (base + 1 - core) * rows + first))

    logits = None
    for array, start in chunks:
        states = lax.dynamic_slice_in_dim(flat, start, array.shape[0], 0)
        term = lax.dot_general(
            states, array, (((0,), (0,)), ((), ())), preferred_element_type=F32
        )
        logits = term if logits is None else logits + term

    columns = vocab * width + jnp.arange(width, dtype=jnp.int32)
    hits = labels[:, None] == columns[None, :]
    peak = jnp.max(logits, axis=1)
    total = jnp.sum(jnp.exp(logits - peak[:, None]), axis=1)
    target = jnp.sum(jnp.where(hits, logits, F32(0.0)), axis=1)
    stats = jnp.stack([peak, total, target])
    stats = combined(gathered(stats, "z", NZ))
    stats = combined(gathered(stats, "y", NY))
    peak, total, target = stats[0], stats[1], stats[2]
    token_loss = jnp.log(total) + peak - target
    shifted = jnp.exp(logits - peak[:, None])
    errors = (shifted / total[:, None] - hits.astype(F32)).astype(BF)

    wide = width // 2
    left, right = errors[:, :wide], errors[:, wide:]
    up_left = shift(left, "x", NX, 1)
    down_right = shift(right, "x", NX, -1)
    up_right = shift(right, "x", NX, 1)
    down_left = shift(left, "x", NX, -1)
    far_left = shift(up_left, "x", NX, 1)
    far_right = shift(down_right, "x", NX, -1)

    terms = jnp.zeros((NY * NZ * part, tokens), BF)
    for array, start in chunks:
        term = lax.dot_general(
            array, errors, (((1,), (1,)), ((), ())), preferred_element_type=F32
        )
        terms = lax.dynamic_update_slice_in_dim(terms, term.astype(BF), start, 0)
    arrived = lax.all_to_all(
        terms.reshape(NY * NZ, part, tokens), ("y", "z"), 0, 0, tiled=True
    )
    state_grad = arrived.astype(F32).sum(axis=0).astype(BF).T

    wanted = lax.dynamic_index_in_dim(
        features.reshape(8, NY, part, tokens), y, 1, keepdims=False
    )
    wanted = lax.all_to_all(wanted, ("x", "core"), 0, 0, tiled=True)
    slices = jnp.concatenate(
        list(gathered(wanted, "y", NY)), axis=1
    )

    def part_grad(block, offset, side):
        who = ((x + offset) % NX) * 2 + side
        states = lax.dynamic_index_in_dim(slices, who, 0, keepdims=False)
        return lax.dot_general(
            states, block, (((1,), (0,)), ((), ())), preferred_element_type=F32
        )

    halves = []
    for blocks in (
        ((left, 0), (up_left, 3), (down_left, 1), (far_left, 2)),
        ((right, 0), (down_right, 1), (up_right, 3), (far_right, 2)),
    ):
        acc = None
        for block, offset in blocks:
            term = part_grad(block, offset, core) + part_grad(swap(block), offset, 1 - core)
            acc = term if acc is None else acc + term
        halves.append(acc)
    head_grad = jnp.concatenate(halves, axis=1)
    return (token_loss, state_grad, head_grad)


def solution(mesh):
    chips = Mesh(mesh.devices.reshape(NX, 2, NY, NZ), ("x", "core", "y", "z"))
    tok, voc = ("x", "core"), ("y", "z")
    in_specs = (P(tok, voc), P(tok, voc), P(tok))
    out_specs = (P(tok), P(tok, voc), P(tok, voc))
    return jax.shard_map(local, mesh=chips, in_specs=in_specs, out_specs=out_specs, check_vma=False)
```

```python
import functools

import jax
import jax.numpy as jnp
from jax import lax
from jax.experimental import pallas as pl
from jax.experimental.pallas import tpu as pltpu
from jax.sharding import Mesh, PartitionSpec as P


BF = jnp.bfloat16
F32 = jnp.float32
NX, NY, NZ = 4, 4, 8


def shift(a, axis, n, s):
    return lax.ppermute(a, axis, [(i, (i + s) % n) for i in range(n)])


def swap(a):
    return lax.ppermute(a, "core", [(0, 1), (1, 0)])


def from_everyone(a, axis, n):
    return lax.all_to_all(jnp.broadcast_to(a[None], (n, *a.shape)), axis, 0, 0, tiled=True)


def combined(parts):
    peaks = parts[:, 0]
    peak = jnp.max(peaks, axis=0)
    total = jnp.sum(parts[:, 1] * jnp.exp(peaks - peak), axis=0)
    return jnp.stack([peak, total, jnp.sum(parts[:, 2], axis=0)])


def logits_kernel(starts, states, *refs, count, more):
    out = refs[-1]
    acc = refs[count][...] if more else None
    for k in range(count):
        rows = refs[k].shape[0]
        start = pl.multiple_of(starts[k], 64)
        term = lax.dot_general(
            states[pl.ds(start, rows), :],
            refs[k][...],
            (((0,), (0,)), ((), ())),
            preferred_element_type=F32,
        )
        acc = term if acc is None else acc + term
    out[...] = acc


def logits_of(states, chunks, acc=None, wide=512):
    arrays = [a for a, _ in chunks]
    starts = jnp.stack([s for _, s in chunks]).astype(jnp.int32)
    depth, tokens = states.shape
    width = arrays[0].shape[1]
    specs = [pl.BlockSpec((depth, tokens), lambda j, s: (0, 0))]
    specs += [pl.BlockSpec((a.shape[0], wide), lambda j, s: (0, j)) for a in arrays]
    tail = []
    if acc is not None:
        specs.append(pl.BlockSpec((tokens, wide), lambda j, s: (0, j)))
        tail = [acc]
    flops = 2 * tokens * width * sum(a.shape[0] for a in arrays)
    return pl.pallas_call(
        functools.partial(logits_kernel, count=len(arrays), more=acc is not None),
        grid_spec=pltpu.PrefetchScalarGridSpec(
            num_scalar_prefetch=1,
            grid=(width // wide,),
            in_specs=specs,
            out_specs=pl.BlockSpec((tokens, wide), lambda j, s: (0, j)),
        ),
        out_shape=jax.ShapeDtypeStruct((tokens, width), F32),
        cost_estimate=pl.CostEstimate(flops=flops, bytes_accessed=flops // 256, transcendentals=0),
        name="logits_part",
    )(starts, states, *arrays, *tail)


def terms_kernel(starts, errors, *refs, count):
    out = refs[-1]
    step = pl.program_id(0)
    for k in range(count):
        rows = refs[k].shape[0]
        start = pl.multiple_of(starts[k] + step * rows, 16)
        out[pl.ds(start, rows), :] = lax.dot_general(
            refs[k][...],
            errors[...],
            (((1,), (1,)), ((), ())),
            preferred_element_type=F32,
        ).astype(BF)


def terms_of(errors, chunks, depth, steps=4):
    arrays = [a for a, _ in chunks]
    starts = jnp.stack([s for _, s in chunks]).astype(jnp.int32)
    tokens, width = errors.shape
    specs = [pl.BlockSpec((tokens, width), lambda j, s: (0, 0))]
    specs += [pl.BlockSpec((a.shape[0] // steps, width), lambda j, s: (j, 0)) for a in arrays]
    flops = 2 * tokens * width * depth
    return pl.pallas_call(
        functools.partial(terms_kernel, count=len(arrays)),
        grid_spec=pltpu.PrefetchScalarGridSpec(
            num_scalar_prefetch=1,
            grid=(steps,),
            in_specs=specs,
            out_specs=pl.BlockSpec((depth, tokens), lambda j, s: (0, 0)),
        ),
        out_shape=jax.ShapeDtypeStruct((depth, tokens), BF),
        cost_estimate=pl.CostEstimate(flops=flops, bytes_accessed=flops // 256, transcendentals=0),
        name="state_terms",
    )(starts, errors, *arrays)


def grad_kernel(who, states, *refs, pairs, halves, more):
    out = refs[-1]
    step = pl.program_id(0)
    acc = refs[-2][...] if more else None
    at = 0
    for k in range(pairs):
        if halves[k]:
            mine, theirs = (
                jnp.where(step < 2, refs[at + i][...], refs[at + 2 + i][...]) for i in (0, 1)
            )
            at += 4
        else:
            mine, theirs = refs[at][...], refs[at + 1][...]
            at += 2
        left = jnp.concatenate([states[who[2 * k]], states[who[2 * k + 1]]], axis=1)
        right = jnp.concatenate([mine, theirs], axis=0)
        term = lax.dot_general(
            left, right, (((1,), (0,)), ((), ())), preferred_element_type=F32
        )
        acc = term if acc is None else acc + term
    out[...] = acc


def grad_of(states, pairs, who, acc=None):
    groups, rows, tokens = states.shape
    blocks = [b for pair in pairs for b in pair]
    width = 2048
    wide = width // 4
    specs = [pl.BlockSpec((groups, rows, tokens), lambda j, s: (0, 0, 0))]
    for pair in pairs:
        if len(pair) == 2:
            specs += [pl.BlockSpec((tokens, wide), lambda j, s: (0, j))] * 2
        else:
            specs += [pl.BlockSpec((tokens, wide), lambda j, s: (0, jnp.minimum(j, 1)))] * 2
            specs += [pl.BlockSpec((tokens, wide), lambda j, s: (0, jnp.maximum(j - 2, 0)))] * 2
    tail = []
    if acc is not None:
        specs.append(pl.BlockSpec((rows, wide), lambda j, s: (0, j)))
        tail = [acc]
    flops = 2 * 2 * tokens * rows * width * len(pairs)
    return pl.pallas_call(
        functools.partial(
            grad_kernel,
            pairs=len(pairs),
            halves=[len(pair) == 4 for pair in pairs],
            more=acc is not None,
        ),
        grid_spec=pltpu.PrefetchScalarGridSpec(
            num_scalar_prefetch=1,
            grid=(4,),
            in_specs=specs,
            out_specs=pl.BlockSpec((rows, wide), lambda j, s: (0, j)),
        ),
        out_shape=jax.ShapeDtypeStruct((rows, width), F32),
        cost_estimate=pl.CostEstimate(flops=flops, bytes_accessed=flops // 256, transcendentals=0),
        name="head_grad_part",
    )(jnp.stack(who).astype(jnp.int32), states, *blocks, *tail)


def step(hidden_states, head, labels):
    x, core, y = lax.axis_index("x"), lax.axis_index("core"), lax.axis_index("y")
    vocab = y * NZ + lax.axis_index("z")
    tokens, part = hidden_states.shape
    rows, width = head.shape
    half = rows // 2
    depth = NY * NZ * part

    low, high = head[:half], head[half:]
    up_low = shift(low, "x", NX, 1)
    down_high = shift(high, "x", NX, -1)
    up_high = shift(high, "x", NX, 1)
    down_low = shift(low, "x", NX, -1)
    partner = swap(head)

    features = from_everyone(hidden_states.T, ("y", "z"), NY * NZ)
    flat = features.reshape(depth, tokens)

    wanted = lax.dynamic_index_in_dim(
        features.reshape(8, NY, part, tokens), y, 1, keepdims=False
    )
    wanted = lax.all_to_all(wanted, ("x", "core"), 0, 0, tiled=True)

    up_low, down_high, _ = lax.optimization_barrier((up_low, down_high, features))
    far_low = shift(up_low, "x", NX, 1)
    far_high = shift(down_high, "x", NX, -1)

    def sides(array, offset, first):
        base = ((x + offset) % NX) * 2
        other = partner if array is head else swap(array)
        return [
            (array, (base + core) * rows + first),
            (other, (base + 1 - core) * rows + first),
        ]

    near = sides(head, 0, 0)
    near += sides(up_low, 3, 0) + sides(down_high, 1, half)
    near += sides(up_high, 3, half) + sides(down_low, 1, 0)
    far = sides(far_low, 2, 0) + sides(far_high, 2, half)

    logits = logits_of(flat, near)
    slices = from_everyone(wanted, "y", NY)
    slices = jnp.moveaxis(slices.reshape(NY, 8, part, tokens), 0, 1).reshape(8, rows, tokens)
    flat, slices = lax.optimization_barrier((flat, slices))
    logits = logits_of(flat, far, logits)

    columns = vocab * width + jnp.arange(width, dtype=jnp.int32)
    hits = labels[:, None] == columns[None, :]
    peak = jnp.max(logits, axis=1)
    total = jnp.sum(jnp.exp(logits - peak[:, None]), axis=1)
    target = jnp.sum(jnp.where(hits, logits, F32(0.0)), axis=1)
    stats = jnp.stack([peak, total, target])
    stats = combined(from_everyone(stats, "z", NZ))
    stats = combined(from_everyone(stats, "y", NY))
    peak, total, target = stats[0], stats[1], stats[2]
    token_loss = jnp.log(total) + peak - target
    shifted = jnp.exp(logits - peak[:, None])
    errors = (shifted / total[:, None] - hits.astype(F32)).astype(BF)

    wide = width // 2
    left, right = errors[:, :wide], errors[:, wide:]
    up_left = shift(left, "x", NX, 1)
    down_right = shift(right, "x", NX, -1)
    up_right = shift(right, "x", NX, 1)
    down_left = shift(left, "x", NX, -1)
    far_left = shift(up_left, "x", NX, 1)
    far_right = shift(down_right, "x", NX, -1)

    terms = terms_of(errors, near + far, depth)
    arrived = lax.all_to_all(
        terms.reshape(NY * NZ, part, tokens), ("y", "z"), 0, 0, tiled=True
    )
    state_grad = arrived.astype(F32).sum(axis=0).astype(BF).T

    def who(offset):
        base = ((x + offset) % NX) * 2
        return [base + core, base + 1 - core]

    other = swap(errors)
    up = (up_left, swap(up_left), up_right, swap(up_right))
    down = (down_left, swap(down_left), down_right, swap(down_right))
    away = (far_left, swap(far_left), far_right, swap(far_right))
    head_grad = grad_of(slices, [(errors, other), up, down], who(0) + who(3) + who(1))
    head_grad = grad_of(slices, [away], who(2), head_grad)
    return (token_loss, state_grad, head_grad)


def solution(mesh):
    chips = Mesh(mesh.devices.reshape(NX, 2, NY, NZ), ("x", "core", "y", "z"))
    tok, voc = ("x", "core"), ("y", "z")
    in_specs = (P(tok, voc), P(tok, voc), P(tok))
    out_specs = (P(tok), P(tok, voc), P(tok, voc))
    return jax.shard_map(step, mesh=chips, in_specs=in_specs, out_specs=out_specs, check_vma=False)
```

```python
import jax
import jax.numpy as jnp
from jax import lax
from jax.experimental import pallas as pl
from jax.experimental.pallas import tpu as pltpu
from jax.sharding import Mesh, PartitionSpec as P


BF = jnp.bfloat16
F32 = jnp.float32
NX, NY, NZ = 4, 4, 8
STEPS = 4


def shift(a, axis, n, s):
    return lax.ppermute(a, axis, [(i, (i + s) % n) for i in range(n)])


def swap(a):
    return lax.ppermute(a, "core", [(0, 1), (1, 0)])


def from_everyone(a, axis, n):
    return lax.all_to_all(jnp.broadcast_to(a[None], (n, *a.shape)), axis, 0, 0, tiled=True)


def ordered(parts, index):
    n = len(parts)
    both = jnp.stack(parts + parts[:-1])
    return lax.dynamic_slice_in_dim(both, (n - index) % n, n, 0)


def dot(a, b):
    return lax.dot_general(a, b, (((1,), (0,)), ((), ())), preferred_element_type=F32)


def whole(a):
    zeros = (0,) * a.ndim
    return pl.BlockSpec(a.shape, lambda j, s: zeros)


def early(j):
    return jnp.minimum(j, STEPS // 2 - 1)


def late(j):
    return jnp.maximum(j - STEPS // 2, 0)


def call(kernel, scalars, args, in_specs, out_specs, out_shape, flops, scratch=()):
    return pl.pallas_call(
        kernel,
        grid_spec=pltpu.PrefetchScalarGridSpec(
            num_scalar_prefetch=1,
            grid=(STEPS,),
            in_specs=in_specs,
            out_specs=out_specs,
            scratch_shapes=scratch,
        ),
        out_shape=out_shape,
        cost_estimate=pl.CostEstimate(flops=flops, bytes_accessed=flops // 256, transcendentals=0),
    )(jnp.stack(scalars).astype(jnp.int32), *args)


def near_kernel(who, states, *refs):
    acc = None
    for k, ref in enumerate(refs[:-1]):
        term = dot(states[who[k]], ref[...])
        acc = term if acc is None else acc + term
    refs[-1][...] = acc


def near_logits(states, arrays, who):
    rows, width = arrays[0].shape
    tokens = states.shape[1]
    wide = width // STEPS
    return call(
        near_kernel,
        who,
        [states, *arrays],
        [whole(states)] + [pl.BlockSpec((rows, wide), lambda j, s: (0, j))] * len(arrays),
        pl.BlockSpec((tokens, wide), lambda j, s: (0, j)),
        jax.ShapeDtypeStruct((tokens, width), F32),
        2 * tokens * rows * width * len(arrays),
    )


def far_kernel(who, states, labels, near, left, left_other, right, right_other, powers, stats, logits):
    step = pl.program_id(0)
    first = step < STEPS // 2
    wide = near.shape[1]
    for mine, theirs, here in ((left, left_other, first), (right, right_other, ~first)):

        @pl.when(here)
        def _():
            logits[:, pl.ds(pl.multiple_of(step * wide, wide), wide)] = (
                near[...] + dot(states[who[0]], mine[...]) + dot(states[who[1]], theirs[...])
            )

    @pl.when(step == STEPS - 1)
    def _():
        values = logits[...]
        peak = jnp.max(values, axis=1, keepdims=True)
        shifted = jnp.exp(values - peak)
        columns = who[2] + lax.broadcasted_iota(jnp.int32, values.shape, 1)
        hits = labels[...] == columns
        total = jnp.sum(shifted, axis=1, keepdims=True)
        target = jnp.sum(jnp.where(hits, values, 0.0), axis=1, keepdims=True)
        powers[...] = shifted.astype(BF)
        lanes = lax.broadcasted_iota(jnp.int32, stats.shape, 1)
        stats[...] = jnp.where(lanes == 0, peak, jnp.where(lanes == 1, total, target))


def far_logits(states, labels, near, left, right, who):
    tokens, width = near.shape
    wide = width // STEPS
    rows = left[0].shape[0]
    args = [states, labels, near, *left, *right]
    specs = [whole(states), whole(labels), pl.BlockSpec((tokens, wide), lambda j, s: (0, j))]
    specs += [pl.BlockSpec((rows, wide), lambda j, s: (0, early(j)))] * 2
    specs += [pl.BlockSpec((rows, wide), lambda j, s: (0, late(j)))] * 2
    powers = jax.ShapeDtypeStruct((tokens, width), BF)
    stats = jax.ShapeDtypeStruct((tokens, 128), F32)
    return call(
        far_kernel,
        who,
        args,
        specs,
        [whole(powers), whole(stats)],
        [powers, stats],
        4 * tokens * rows * width,
        [pltpu.VMEM((tokens, width), F32)],
    )


def terms_kernel(starts, powers, labels, *refs):
    *arrays, sums, picks, both = refs
    step = pl.program_id(0)
    width, double = both.shape
    tokens = double // 2

    @pl.when(step == 0)
    def _():
        both[:, :tokens] = powers[...].T
        columns = starts[8] + lax.broadcasted_iota(jnp.int32, (width, tokens), 0)
        both[:, tokens:] = jnp.where(columns == labels[...], 1.0, 0.0).astype(BF)

    def put(k, term):
        rows = term.shape[0]
        at = pl.ds(pl.multiple_of(starts[k] + step * rows, 32), rows)
        sums[at, :] = term[:, :tokens]
        picks[at, :] = term[:, tokens:].astype(BF)

    for k in range(6):
        put(k, dot(arrays[k][...], both[...]))
    half = width // 2
    for k in range(2):
        left, right = arrays[6 + k], arrays[8 + k]
        put(6 + k, dot(left[...], both[:half, :]) + dot(right[...], both[half:, :]))


def state_terms(powers, labels, near, left, right, starts, depth):
    tokens, width = powers.shape
    rows = near[0].shape[0] // STEPS
    args = [powers, labels, *near, *left, *right]
    specs = [whole(powers), whole(labels)]
    specs += [pl.BlockSpec((rows, a.shape[1]), lambda j, s: (j, 0)) for a in args[2:]]
    sums = jax.ShapeDtypeStruct((depth, tokens), F32)
    picks = jax.ShapeDtypeStruct((depth, tokens), BF)
    return call(
        terms_kernel,
        starts,
        args,
        specs,
        [whole(sums), whole(picks)],
        [sums, picks],
        4 * tokens * width * depth,
        [pltpu.VMEM((width, 2 * tokens), BF)],
    )


def grad_kernel(who, states, scales, labels, *refs):
    *arrays, out = refs
    step = pl.program_id(0)
    tokens = states.shape[2]
    wide = out.shape[1]
    columns = who[8] + step * wide + lax.broadcasted_iota(jnp.int32, (tokens, wide), 1)
    blocks = [a[...] for a in arrays[:6]]
    first = step < STEPS // 2
    blocks += [jnp.where(first, arrays[6 + k][...], arrays[8 + k][...]) for k in range(2)]
    acc = None
    for pair in range(4):
        left, right = [], []
        for k in (2 * pair, 2 * pair + 1):
            wanted = labels[pl.ds(pl.multiple_of(who[k] * tokens, tokens), tokens), :]
            hit = jnp.where(wanted == columns, 1.0, 0.0)
            scale = scales[k * tokens : (k + 1) * tokens, :]
            right.append((blocks[k].astype(F32) * scale - hit).astype(BF))
            left.append(states[who[k]])
        term = dot(jnp.concatenate(left, axis=1), jnp.concatenate(right, axis=0))
        acc = term if acc is None else acc + term
    out[...] = acc


def head_grad_of(states, scales, labels, near, left, right, who):
    groups, rows, tokens = states.shape
    width = near[0].shape[1]
    wide = width // STEPS
    args = [states, scales, labels, *near, *left, *right]
    specs = [whole(states), whole(scales), whole(labels)]
    specs += [pl.BlockSpec((tokens, wide), lambda j, s: (0, j))] * 6
    specs += [pl.BlockSpec((tokens, wide), lambda j, s: (0, early(j)))] * 2
    specs += [pl.BlockSpec((tokens, wide), lambda j, s: (0, late(j)))] * 2
    return call(
        grad_kernel,
        who,
        args,
        specs,
        pl.BlockSpec((rows, wide), lambda j, s: (0, j)),
        jax.ShapeDtypeStruct((rows, width), F32),
        2 * groups * tokens * rows * width,
    )


def step(hidden_states, head, labels):
    x, core, y = lax.axis_index("x"), lax.axis_index("core"), lax.axis_index("y")
    vocab = y * NZ + lax.axis_index("z")
    tokens, part = hidden_states.shape
    rows, width = head.shape
    half = width // 2
    depth = NY * NZ * part
    base = vocab * width

    def who(offset):
        chip = ((x + offset) % NX) * 2
        return [chip + core, chip + 1 - core]

    up = shift(head, "x", NX, 1)
    down = shift(head, "x", NX, -1)
    partner = swap(head)
    far_left = shift(up[:, :half], "x", NX, 1)
    far_right = shift(down[:, half:], "x", NX, -1)
    near = [head, partner, up, swap(up), down, swap(down)]
    left = [far_left, swap(far_left)]
    right = [far_right, swap(far_right)]

    features = from_everyone(hidden_states.T, ("y", "z"), NY * NZ)
    flat = jnp.swapaxes(features.reshape(8, rows, tokens), 1, 2)

    wanted = lax.dynamic_index_in_dim(
        features.reshape(8, NY, part, tokens), y, 1, keepdims=False
    )
    digits = jnp.stack([labels // 256, labels % 256]).astype(BF)
    digits = jnp.broadcast_to(jnp.pad(digits, ((0, 14), (0, 0)))[None], (8, 16, tokens))
    wanted = lax.all_to_all(
        jnp.concatenate([wanted, digits], axis=1), ("x", "core"), 0, 0, tiled=True
    )
    digits = wanted[:, part : part + 2].astype(jnp.int32)
    all_labels = (digits[:, 0] * 256 + digits[:, 1]).reshape(8 * tokens, 1)
    wanted = wanted[:, :part]

    logits = near_logits(flat, near, who(0) + who(3) + who(1))
    powers, stats = far_logits(
        flat, labels[:, None], logits, left, right, who(2) + [base]
    )
    stats = stats.T[:3]

    pow_up = shift(powers, "x", NX, 1)
    pow_down = shift(powers, "x", NX, -1)
    pow_left = shift(pow_up[:, :half], "x", NX, 1)
    pow_right = shift(pow_down[:, half:], "x", NX, -1)
    pow_near = [powers, swap(powers), pow_up, swap(pow_up), pow_down, swap(pow_down)]
    pow_left = [pow_left, swap(pow_left)]
    pow_right = [pow_right, swap(pow_right)]

    parts = from_everyone(stats, ("y", "z"), NY * NZ)
    starts = [w * rows for w in who(0) + who(3) + who(1) + who(2)]
    sums, picks = state_terms(
        powers, labels[None], near, left, right, starts + [base], depth
    )
    peak = jnp.max(parts[:, 0], axis=0)
    total = jnp.sum(parts[:, 1] * jnp.exp(parts[:, 0] - peak), axis=0)
    target = jnp.sum(parts[:, 2], axis=0)
    token_loss = jnp.log(total) + peak - target
    scale = jnp.exp(stats[0] - peak) / total

    terms = (sums * scale - picks.astype(F32)).astype(BF)
    arrived = lax.all_to_all(
        terms.reshape(NY * NZ, part, tokens), ("y", "z"), 0, 0, tiled=True
    )
    state_grad = arrived.astype(F32).sum(axis=0).astype(BF).T

    slices = ordered([wanted] + [shift(wanted, "y", NY, -j) for j in (1, 2, 3)], y)
    slices = jnp.swapaxes(slices, 0, 1).reshape(8, rows, tokens)
    scale = jnp.stack([scale, swap(scale)])
    scales = [scale] + [shift(scale, "x", NX, s) for s in (1, -1, 2)]
    scales = jnp.concatenate(scales).reshape(8 * tokens, 1)
    head_grad = head_grad_of(
        slices,
        scales,
        all_labels,
        pow_near,
        pow_left,
        pow_right,
        who(0) + who(3) + who(1) + who(2) + [base],
    )
    return (token_loss, state_grad, head_grad)


def solution(mesh):
    chips = Mesh(mesh.devices.reshape(NX, 2, NY, NZ), ("x", "core", "y", "z"))
    tok, voc = ("x", "core"), ("y", "z")
    in_specs = (P(tok, voc), P(tok, voc), P(tok))
    out_specs = (P(tok), P(tok, voc), P(tok, voc))
    return jax.shard_map(step, mesh=chips, in_specs=in_specs, out_specs=out_specs, check_vma=False)
```

```python
import jax
import jax.numpy as jnp
from jax import lax
from jax.experimental import pallas as pl
from jax.experimental.pallas import tpu as pltpu
from jax.sharding import Mesh, PartitionSpec as P


BF = jnp.bfloat16
F32 = jnp.float32
NX, NY, NZ = 4, 4, 8
STEPS = 4


def shift(a, axis, n, s):
    return lax.ppermute(a, axis, [(i, (i + s) % n) for i in range(n)])


def swap(a):
    return lax.ppermute(a, "core", [(0, 1), (1, 0)])


def from_everyone(a, axis, n):
    return lax.all_to_all(jnp.broadcast_to(a[None], (n, *a.shape)), axis, 0, 0, tiled=True)


def ordered(parts, index):
    n = len(parts)
    both = jnp.stack(parts + parts[:-1])
    return lax.dynamic_slice_in_dim(both, (n - index) % n, n, 0)


def dot(a, b):
    return lax.dot_general(a, b, (((1,), (0,)), ((), ())), preferred_element_type=F32)


def whole(a):
    zeros = (0,) * a.ndim
    return pl.BlockSpec(a.shape, lambda j, s: zeros)


def early(j):
    return jnp.minimum(j, STEPS // 2 - 1)


def late(j):
    return jnp.maximum(j - STEPS // 2, 0)


def call(kernel, scalars, args, in_specs, out_specs, out_shape, flops, scratch=()):
    return pl.pallas_call(
        kernel,
        grid_spec=pltpu.PrefetchScalarGridSpec(
            num_scalar_prefetch=1,
            grid=(STEPS,),
            in_specs=in_specs,
            out_specs=out_specs,
            scratch_shapes=scratch,
        ),
        out_shape=out_shape,
        cost_estimate=pl.CostEstimate(flops=flops, bytes_accessed=flops // 256, transcendentals=0),
    )(jnp.stack(scalars).astype(jnp.int32), *args)


def near_kernel(who, states, *refs):
    *arrays, out = refs
    first = pl.program_id(0) < STEPS // 2

    def total(chosen):
        acc = None
        for k, ref in enumerate(chosen):
            term = dot(states[who[k]], ref[...])
            acc = term if acc is None else acc + term
        return acc

    @pl.when(first)
    def _():
        out[...] = total(arrays[:6])

    @pl.when(~first)
    def _():
        out[...] = total(arrays[:2] + arrays[6:])


def near_logits(states, own, left, right, who):
    rows, width = own[0].shape
    tokens = states.shape[1]
    wide = width // STEPS
    specs = [whole(states)] + [pl.BlockSpec((rows, wide), lambda j, s: (0, j))] * 2
    specs += [pl.BlockSpec((rows, wide), lambda j, s: (0, early(j)))] * 4
    specs += [pl.BlockSpec((rows, wide), lambda j, s: (0, late(j)))] * 4
    return call(
        near_kernel,
        who,
        [states, *own, *left, *right],
        specs,
        pl.BlockSpec((tokens, wide), lambda j, s: (0, j)),
        jax.ShapeDtypeStruct((tokens, width), F32),
        12 * tokens * rows * width,
    )


def far_kernel(who, mine_states, other_states, labels, near, left, left_other, right, right_other, powers, stats, logits):
    step = pl.program_id(0)
    first = step < STEPS // 2
    wide = near.shape[1]
    for mine, theirs, here in ((left, left_other, first), (right, right_other, ~first)):

        @pl.when(here)
        def _():
            logits[:, pl.ds(pl.multiple_of(step * wide, wide), wide)] = (
                near[...] + dot(mine_states[0], mine[...]) + dot(other_states[0], theirs[...])
            )

    @pl.when(step == STEPS - 1)
    def _():
        values = logits[...]
        peak = jnp.max(values, axis=1, keepdims=True)
        shifted = jnp.exp(values - peak)
        columns = who[2] + lax.broadcasted_iota(jnp.int32, values.shape, 1)
        hits = labels[...] == columns
        total = jnp.sum(shifted, axis=1, keepdims=True)
        target = jnp.sum(jnp.where(hits, values, 0.0), axis=1, keepdims=True)
        powers[...] = shifted.astype(BF)
        tokens = values.shape[0]
        lanes = lax.broadcasted_iota(jnp.int32, (tokens, 128), 1)
        both = jnp.where(lanes == 0, peak, jnp.where(lanes == 1, total, target))
        stats[...] = both.T[:8]


def far_logits(states, labels, near, left, right, who):
    tokens, width = near.shape
    wide = width // STEPS
    rows = left[0].shape[0]
    args = [states, states, labels, near, *left, *right]
    specs = [pl.BlockSpec((1, tokens, rows), lambda j, s, k=k: (s[k], 0, 0)) for k in (0, 1)]
    specs += [whole(labels), pl.BlockSpec((tokens, wide), lambda j, s: (0, j))]
    specs += [pl.BlockSpec((rows, wide), lambda j, s: (0, early(j)))] * 2
    specs += [pl.BlockSpec((rows, wide), lambda j, s: (0, late(j)))] * 2
    powers = jax.ShapeDtypeStruct((tokens, width), BF)
    stats = jax.ShapeDtypeStruct((8, 128), F32)
    return call(
        far_kernel,
        who,
        args,
        specs,
        [whole(powers), whole(stats)],
        [powers, stats],
        4 * tokens * rows * width,
        [pltpu.VMEM((tokens, width), F32)],
    )


def terms_kernel(starts, powers, labels, *refs):
    *arrays, sums, picks, both = refs
    step = pl.program_id(0)
    width, double = both.shape
    tokens = double // 2

    @pl.when(step == 0)
    def _():
        both[:, :tokens] = powers[...].T
        columns = starts[8] + lax.broadcasted_iota(jnp.int32, (width, tokens), 0)
        both[:, tokens:] = jnp.where(columns == labels[...], 1.0, 0.0).astype(BF)

    half = width // 2
    own, left, right = arrays[:2], arrays[2:8], arrays[8:]
    lefts = jnp.concatenate([a[:, :half] for a in own] + [a[...] for a in left], axis=0)
    rights = jnp.concatenate([a[:, half:] for a in own] + [a[...] for a in right], axis=0)
    term = dot(lefts, both[:half, :]) + dot(rights, both[half:, :])
    rows = own[0].shape[0]
    for k in range(8):
        at = pl.ds(pl.multiple_of(starts[k] + step * rows, 32), rows)
        sums[at, :] = term[k * rows : (k + 1) * rows, :tokens]
        picks[at, :] = term[k * rows : (k + 1) * rows, tokens:].astype(BF)


def state_terms(powers, labels, own, left, right, starts, depth):
    tokens, width = powers.shape
    rows = own[0].shape[0] // STEPS
    args = [powers, labels, *own, *left, *right]
    specs = [whole(powers), whole(labels)]
    specs += [pl.BlockSpec((rows, a.shape[1]), lambda j, s: (j, 0)) for a in args[2:]]
    sums = jax.ShapeDtypeStruct((depth, tokens), F32)
    picks = jax.ShapeDtypeStruct((depth, tokens), BF)
    return call(
        terms_kernel,
        starts,
        args,
        specs,
        [whole(sums), whole(picks)],
        [sums, picks],
        4 * tokens * width * depth,
        [pltpu.VMEM((width, 2 * tokens), BF)],
    )


def grad_kernel(who, p0, p1, p2, p3, scales, labels, *refs):
    *arrays, out, states = refs
    step = pl.program_id(0)
    groups, part, tokens = p0.shape
    wide = out.shape[1]

    @pl.when(step == 0)
    def _():
        for j, parts in enumerate((p0, p1, p2, p3)):
            at = pl.multiple_of(((who[9] + j) % NY) * part, 32)
            for k in range(groups):
                states[k, pl.ds(at, part), :] = parts[k]

    columns = who[8] + step * wide + lax.broadcasted_iota(jnp.int32, (tokens, wide), 1)
    blocks = [a[...] for a in arrays[:6]]
    first = step < STEPS // 2
    blocks += [jnp.where(first, arrays[6 + k][...], arrays[8 + k][...]) for k in range(2)]
    acc = None
    for pair in range(4):
        left, right = [], []
        for k in (2 * pair, 2 * pair + 1):
            wanted = labels[pl.ds(pl.multiple_of(who[k] * tokens, tokens), tokens), :]
            hit = jnp.where(wanted == columns, 1.0, 0.0)
            scale = scales[k * tokens : (k + 1) * tokens, :]
            right.append((blocks[k].astype(F32) * scale - hit).astype(BF))
            left.append(states[who[k]])
        term = dot(jnp.concatenate(left, axis=1), jnp.concatenate(right, axis=0))
        acc = term if acc is None else acc + term
    out[...] = acc


def head_grad_of(parts, scales, labels, near, left, right, who):
    groups, part, tokens = parts[0].shape
    rows = NY * part
    width = near[0].shape[1]
    wide = width // STEPS
    args = [*parts, scales, labels, *near, *left, *right]
    specs = [whole(a) for a in args[:6]]
    specs += [pl.BlockSpec((tokens, wide), lambda j, s: (0, j))] * 6
    specs += [pl.BlockSpec((tokens, wide), lambda j, s: (0, early(j)))] * 2
    specs += [pl.BlockSpec((tokens, wide), lambda j, s: (0, late(j)))] * 2
    return call(
        grad_kernel,
        who,
        args,
        specs,
        pl.BlockSpec((rows, wide), lambda j, s: (0, j)),
        jax.ShapeDtypeStruct((rows, width), F32),
        2 * groups * tokens * rows * width,
        [pltpu.VMEM((groups, rows, tokens), BF)],
    )


def step(hidden_states, head, labels):
    x, core, y = lax.axis_index("x"), lax.axis_index("core"), lax.axis_index("y")
    vocab = y * NZ + lax.axis_index("z")
    tokens, part = hidden_states.shape
    rows, width = head.shape
    half = width // 2
    depth = NY * NZ * part
    base = vocab * width

    def who(offset):
        chip = ((x + offset) % NX) * 2
        return [chip + core, chip + 1 - core]

    up_left = shift(head[:, :half], "x", NX, 1)
    down_right = shift(head[:, half:], "x", NX, -1)
    up_right = shift(head[:, half:], "x", NX, 1)
    down_left = shift(head[:, :half], "x", NX, -1)
    own = [head, swap(head)]
    far_left = shift(up_left, "x", NX, 1)
    far_right = shift(down_right, "x", NX, -1)
    left = [up_left, swap(up_left), down_left, swap(down_left)]
    right = [up_right, swap(up_right), down_right, swap(down_right)]
    away_left = [far_left, swap(far_left)]
    away_right = [far_right, swap(far_right)]

    row = from_everyone(hidden_states.T, "z", NZ)
    parts = [row] + [shift(row, "y", NY, -j) for j in (1, 2, 3)]
    flat = jnp.stack(parts).reshape(8, rows, tokens)
    flat = jnp.swapaxes(flat, 1, 2)

    def block(offset):
        chip = ((x + offset - y) % NY) * 2
        return [chip + core, chip + 1 - core]

    picked = [
        lax.dynamic_index_in_dim(p.reshape(2, NY, part, tokens), y, 1, keepdims=False)
        for p in parts
    ]
    wanted = ordered(picked, y).reshape(8, part, tokens)
    digits = jnp.stack([labels // 256, labels % 256]).astype(BF)
    digits = jnp.broadcast_to(jnp.pad(digits, ((0, 14), (0, 0)))[None], (8, 16, tokens))
    wanted = lax.all_to_all(
        jnp.concatenate([wanted, digits], axis=1), ("x", "core"), 0, 0, tiled=True
    )
    far_states, wanted = lax.optimization_barrier((flat, wanted))
    digits = wanted[:, part : part + 2].astype(jnp.int32)
    all_labels = (digits[:, 0] * 256 + digits[:, 1]).reshape(8 * tokens, 1)
    wanted = wanted[:, :part]

    logits = near_logits(flat, own, left, right, block(0) + block(3) + block(1))
    powers, stats = far_logits(
        far_states, labels[:, None], logits, away_left, away_right, block(2) + [base]
    )

    pow_up = shift(powers, "x", NX, 1)
    pow_down = shift(powers, "x", NX, -1)
    pow_left = shift(pow_up[:, :half], "x", NX, 1)
    pow_right = shift(pow_down[:, half:], "x", NX, -1)
    pow_near = [powers, swap(powers), pow_up, swap(pow_up), pow_down, swap(pow_down)]
    pow_left = [pow_left, swap(pow_left)]
    pow_right = [pow_right, swap(pow_right)]

    parts = from_everyone(stats[:3], ("y", "z"), NY * NZ)
    starts = [w * rows for w in who(0) + who(3) + who(1) + who(2)]
    sums, picks = state_terms(
        powers, labels[None], own, left + away_left, right + away_right, starts + [base], depth
    )
    peak = jnp.max(parts[:, 0], axis=0)
    total = jnp.sum(parts[:, 1] * jnp.exp(parts[:, 0] - peak), axis=0)
    target = jnp.sum(parts[:, 2], axis=0)
    token_loss = jnp.log(total) + peak - target
    scale = jnp.exp(stats[0] - peak) / total

    terms = (sums * scale - picks.astype(F32)).astype(BF)
    arrived = lax.all_to_all(
        terms.reshape(NY * NZ, part, tokens), ("y", "z"), 0, 0, tiled=True
    )
    state_grad = arrived.astype(F32).sum(axis=0).astype(BF).T

    slices = [wanted] + [shift(wanted, "y", NY, -j) for j in (1, 2, 3)]
    scale = jnp.stack([scale, swap(scale)])
    scales = [scale] + [shift(scale, "x", NX, s) for s in (1, -1, 2)]
    scales = jnp.concatenate(scales).reshape(8 * tokens, 1)
    head_grad = head_grad_of(
        slices,
        scales,
        all_labels,
        pow_near,
        pow_left,
        pow_right,
        who(0) + who(3) + who(1) + who(2) + [base, y],
    )
    return (token_loss, state_grad, head_grad)


def solution(mesh):
    chips = Mesh(mesh.devices.reshape(NX, 2, NY, NZ), ("x", "core", "y", "z"))
    tok, voc = ("x", "core"), ("y", "z")
    in_specs = (P(tok, voc), P(tok, voc), P(tok))
    out_specs = (P(tok), P(tok, voc), P(tok, voc))
    return jax.shard_map(step, mesh=chips, in_specs=in_specs, out_specs=out_specs, check_vma=False)
```

```python
import jax
import jax.numpy as jnp
from jax import lax
from jax.experimental import pallas as pl
from jax.experimental.pallas import tpu as pltpu
from jax.sharding import Mesh, PartitionSpec as P


BF = jnp.bfloat16
F32 = jnp.float32
NX, NY, NZ = 4, 4, 8
STEPS = 4


def shift(a, axis, n, s):
    return lax.ppermute(a, axis, [(i, (i + s) % n) for i in range(n)])


def swap(a):
    return lax.ppermute(a, "core", [(0, 1), (1, 0)])


def from_everyone(a, axis, n):
    return lax.all_to_all(jnp.broadcast_to(a[None], (n, *a.shape)), axis, 0, 0, tiled=True)


def dot(a, b):
    return lax.dot_general(a, b, (((1,), (0,)), ((), ())), preferred_element_type=F32)


def whole(a):
    zeros = (0,) * a.ndim
    return pl.BlockSpec(a.shape, lambda j, s: zeros)


def early(j):
    return jnp.minimum(j, STEPS // 2 - 1)


def late(j):
    return jnp.maximum(j - STEPS // 2, 0)


def call(kernel, scalars, args, in_specs, out_specs, out_shape, flops, scratch=(), steps=STEPS):
    return pl.pallas_call(
        kernel,
        grid_spec=pltpu.PrefetchScalarGridSpec(
            num_scalar_prefetch=1,
            grid=(steps,),
            in_specs=in_specs,
            out_specs=out_specs,
            scratch_shapes=scratch,
        ),
        out_shape=out_shape,
        cost_estimate=pl.CostEstimate(flops=flops, bytes_accessed=flops // 256, transcendentals=0),
    )(jnp.stack(scalars).astype(jnp.int32), *args)


def prepare_kernel(who, p0, p1, p2, p3, digits, states, wanted):
    part = p0.shape[1]
    for j, parts in enumerate((p0, p1, p2, p3)):
        chip = (who[0] + j) % NY
        for c in range(2):
            rows = parts[4 * c : 4 * c + 4].reshape(4 * part, -1)
            states[2 * chip + c] = rows.T
            wanted[2 * chip + c, :part, :] = parts[4 * c + who[0]]
            wanted[2 * chip + c, part:, :] = digits[...]


def prepared(parts, digits, y):
    _, part, tokens = parts[0].shape
    states = jax.ShapeDtypeStruct((8, tokens, 4 * part), BF)
    wanted = jax.ShapeDtypeStruct((8, part + 16, tokens), BF)
    args = [*parts, digits]
    return call(
        prepare_kernel,
        [y, y],
        args,
        [whole(a) for a in args],
        [whole(states), whole(wanted)],
        [states, wanted],
        1 << 20,
        steps=1,
    )


def near_kernel(who, states, *refs):
    *arrays, out = refs
    first = pl.program_id(0) < STEPS // 2

    def total(chosen):
        acc = None
        for k, ref in enumerate(chosen):
            term = dot(states[who[k]], ref[...])
            acc = term if acc is None else acc + term
        return acc

    @pl.when(first)
    def _():
        out[...] = total(arrays[:6])

    @pl.when(~first)
    def _():
        out[...] = total(arrays[:2] + arrays[6:])


def near_logits(states, own, left, right, who):
    rows, width = own[0].shape
    tokens = states.shape[1]
    wide = width // STEPS
    specs = [whole(states)] + [pl.BlockSpec((rows, wide), lambda j, s: (0, j))] * 2
    specs += [pl.BlockSpec((rows, wide), lambda j, s: (0, early(j)))] * 4
    specs += [pl.BlockSpec((rows, wide), lambda j, s: (0, late(j)))] * 4
    return call(
        near_kernel,
        who,
        [states, *own, *left, *right],
        specs,
        pl.BlockSpec((tokens, wide), lambda j, s: (0, j)),
        jax.ShapeDtypeStruct((tokens, width), F32),
        12 * tokens * rows * width,
    )


def far_kernel(who, mine_states, other_states, labels, near, left, left_other, right, right_other, powers, stats, logits):
    step = pl.program_id(0)
    first = step < STEPS // 2
    wide = near.shape[1]
    for mine, theirs, here in ((left, left_other, first), (right, right_other, ~first)):

        @pl.when(here)
        def _():
            logits[:, pl.ds(pl.multiple_of(step * wide, wide), wide)] = (
                near[...] + dot(mine_states[0], mine[...]) + dot(other_states[0], theirs[...])
            )

    @pl.when(step == STEPS - 1)
    def _():
        values = logits[...]
        peak = jnp.max(values, axis=1, keepdims=True)
        shifted = jnp.exp(values - peak)
        columns = who[2] + lax.broadcasted_iota(jnp.int32, values.shape, 1)
        hits = labels[...] == columns
        total = jnp.sum(shifted, axis=1, keepdims=True)
        target = jnp.sum(jnp.where(hits, values, 0.0), axis=1, keepdims=True)
        powers[...] = shifted.astype(BF)
        tokens = values.shape[0]
        lanes = lax.broadcasted_iota(jnp.int32, (tokens, 128), 1)
        both = jnp.where(lanes == 0, peak, jnp.where(lanes == 1, total, target))
        stats[...] = both.T[:8]


def far_logits(states, labels, near, left, right, who):
    tokens, width = near.shape
    wide = width // STEPS
    rows = left[0].shape[0]
    args = [states, states, labels, near, *left, *right]
    specs = [pl.BlockSpec((1, tokens, rows), lambda j, s, k=k: (s[k], 0, 0)) for k in (0, 1)]
    specs += [whole(labels), pl.BlockSpec((tokens, wide), lambda j, s: (0, j))]
    specs += [pl.BlockSpec((rows, wide), lambda j, s: (0, early(j)))] * 2
    specs += [pl.BlockSpec((rows, wide), lambda j, s: (0, late(j)))] * 2
    powers = jax.ShapeDtypeStruct((tokens, width), BF)
    stats = jax.ShapeDtypeStruct((8, 128), F32)
    return call(
        far_kernel,
        who,
        args,
        specs,
        [whole(powers), whole(stats)],
        [powers, stats],
        4 * tokens * rows * width,
        [pltpu.VMEM((tokens, width), F32)],
    )


def terms_kernel(starts, powers, labels, *refs):
    *arrays, sums, picks, both = refs
    step = pl.program_id(0)
    width, double = both.shape
    tokens = double // 2

    @pl.when(step == 0)
    def _():
        both[:, :tokens] = powers[...].T
        columns = starts[8] + lax.broadcasted_iota(jnp.int32, (width, tokens), 0)
        both[:, tokens:] = jnp.where(columns == labels[...], 1.0, 0.0).astype(BF)

    half = width // 2
    own, left, right = arrays[:2], arrays[2:8], arrays[8:]
    lefts = jnp.concatenate([a[:, :half] for a in own] + [a[...] for a in left], axis=0)
    rights = jnp.concatenate([a[:, half:] for a in own] + [a[...] for a in right], axis=0)
    term = dot(lefts, both[:half, :]) + dot(rights, both[half:, :])
    rows = own[0].shape[0]
    for k in range(8):
        at = pl.ds(pl.multiple_of(starts[k] + step * rows, 32), rows)
        sums[at, :] = term[k * rows : (k + 1) * rows, :tokens]
        picks[at, :] = term[k * rows : (k + 1) * rows, tokens:].astype(BF)


def state_terms(powers, labels, own, left, right, starts, depth):
    tokens, width = powers.shape
    rows = own[0].shape[0] // STEPS
    args = [powers, labels, *own, *left, *right]
    specs = [whole(powers), whole(labels)]
    specs += [pl.BlockSpec((rows, a.shape[1]), lambda j, s: (j, 0)) for a in args[2:]]
    sums = jax.ShapeDtypeStruct((depth, tokens), F32)
    picks = jax.ShapeDtypeStruct((depth, tokens), BF)
    return call(
        terms_kernel,
        starts,
        args,
        specs,
        [whole(sums), whole(picks)],
        [sums, picks],
        4 * tokens * width * depth,
        [pltpu.VMEM((width, 2 * tokens), BF)],
    )


def grad_kernel(who, p0, p1, p2, p3, scales, *refs):
    *arrays, out, states, turned = refs
    step = pl.program_id(0)
    groups, padded, tokens = p0.shape
    part = padded - 16
    wide = out.shape[1]

    @pl.when(step == 0)
    def _():
        for j, parts in enumerate((p0, p1, p2, p3)):
            at = pl.multiple_of(((who[9] + j) % NY) * part, 32)
            for k in range(groups):
                states[k, pl.ds(at, part), :] = parts[k, :part, :]
        for k in range(groups):
            digits = p0[who[k], part:, :].astype(F32)
            number = digits[0:1] * 256.0 + digits[1:2]
            both = jnp.concatenate([number, scales[k : k + 1, :], digits[:6]], axis=0)
            turned[k] = both.T

    columns = who[8] + step * wide + lax.broadcasted_iota(jnp.int32, (tokens, wide), 1)
    columns = columns.astype(F32)
    blocks = [a[...] for a in arrays[:6]]
    first = step < STEPS // 2
    blocks += [jnp.where(first, arrays[6 + k][...], arrays[8 + k][...]) for k in range(2)]
    acc = None
    for pair in range(4):
        left, right = [], []
        for k in (2 * pair, 2 * pair + 1):
            hit = jnp.where(turned[k][:, 0:1] == columns, 1.0, 0.0)
            right.append((blocks[k].astype(F32) * turned[k][:, 1:2] - hit).astype(BF))
            left.append(states[who[k]])
        term = dot(jnp.concatenate(left, axis=1), jnp.concatenate(right, axis=0))
        acc = term if acc is None else acc + term
    out[...] = acc


def head_grad_of(parts, scales, near, left, right, who):
    groups, padded, tokens = parts[0].shape
    rows = NY * (padded - 16)
    width = near[0].shape[1]
    wide = width // STEPS
    args = [*parts, scales, *near, *left, *right]
    specs = [whole(a) for a in args[:5]]
    specs += [pl.BlockSpec((tokens, wide), lambda j, s: (0, j))] * 6
    specs += [pl.BlockSpec((tokens, wide), lambda j, s: (0, early(j)))] * 2
    specs += [pl.BlockSpec((tokens, wide), lambda j, s: (0, late(j)))] * 2
    return call(
        grad_kernel,
        who,
        args,
        specs,
        pl.BlockSpec((rows, wide), lambda j, s: (0, j)),
        jax.ShapeDtypeStruct((rows, width), F32),
        2 * groups * tokens * rows * width,
        [pltpu.VMEM((groups, rows, tokens), BF), pltpu.VMEM((groups, tokens, 8), F32)],
    )


def step(hidden_states, head, labels):
    x, core, y = lax.axis_index("x"), lax.axis_index("core"), lax.axis_index("y")
    vocab = y * NZ + lax.axis_index("z")
    tokens, part = hidden_states.shape
    rows, width = head.shape
    half = width // 2
    depth = NY * NZ * part
    base = vocab * width

    def who(offset):
        chip = ((x + offset) % NX) * 2
        return [chip + core, chip + 1 - core]

    up_left = shift(head[:, :half], "x", NX, 1)
    down_right = shift(head[:, half:], "x", NX, -1)
    up_right = shift(head[:, half:], "x", NX, 1)
    down_left = shift(head[:, :half], "x", NX, -1)
    own = [head, swap(head)]
    far_left = shift(up_left, "x", NX, 1)
    far_right = shift(down_right, "x", NX, -1)
    up_left_other, down_right_other = swap(up_left), swap(down_right)
    left = [up_left, up_left_other, down_left, swap(down_left)]
    right = [up_right, swap(up_right), down_right, down_right_other]
    away_left = [far_left, swap(far_left)]
    away_right = [far_right, swap(far_right)]

    row = from_everyone(hidden_states.T, "z", NZ)
    parts = [row] + [shift(row, "y", NY, -j) for j in (1, 2, 3)]
    digits = jnp.stack([labels // 256, labels % 256]).astype(BF)
    digits = jnp.pad(digits, ((0, 14), (0, 0)))
    states, wanted = prepared(parts, digits, y)
    wanted = lax.all_to_all(wanted, ("x", "core"), 0, 0, tiled=True)
    far_states, wanted = lax.optimization_barrier((states, wanted))

    slices = [wanted] + [shift(wanted, "y", NY, -j) for j in (1, 2, 3)]
    logits = near_logits(states, own, left, right, who(0) + who(3) + who(1))
    powers, stats = far_logits(
        far_states, labels[:, None], logits, away_left, away_right, who(2) + [base]
    )

    pow_up = shift(powers, "x", NX, 1)
    pow_down = shift(powers, "x", NX, -1)
    pow_left = shift(pow_up[:, :half], "x", NX, 1)
    pow_right = shift(pow_down[:, half:], "x", NX, -1)
    pow_near = [powers, swap(powers), pow_up, swap(pow_up), pow_down, swap(pow_down)]
    pow_left = [pow_left, swap(pow_left)]
    pow_right = [pow_right, swap(pow_right)]

    parts = from_everyone(stats[:3], ("y", "z"), NY * NZ)
    starts = [w * rows for w in who(0) + who(3) + who(1) + who(2)]
    sums, picks = state_terms(
        powers, labels[None], own, left + away_left, right + away_right, starts + [base], depth
    )
    peak = jnp.max(parts[:, 0], axis=0)
    total = jnp.sum(parts[:, 1] * jnp.exp(parts[:, 0] - peak), axis=0)
    target = jnp.sum(parts[:, 2], axis=0)
    token_loss = jnp.log(total) + peak - target
    scale = jnp.exp(stats[0] - peak) / total

    terms = (sums * scale - picks.astype(F32)).astype(BF)
    arrived = lax.all_to_all(
        terms.reshape(NY * NZ, part, tokens), ("y", "z"), 0, 0, tiled=True
    )
    state_grad = arrived.astype(F32).sum(axis=0).astype(BF).T

    scale = jnp.stack([scale, swap(scale)])
    scales = [scale] + [shift(scale, "x", NX, s) for s in (1, -1, 2)]
    scales = jnp.concatenate(scales)
    head_grad = head_grad_of(
        slices,
        scales,
        pow_near,
        pow_left,
        pow_right,
        who(0) + who(3) + who(1) + who(2) + [base, y],
    )
    return (token_loss, state_grad, head_grad)


def solution(mesh):
    chips = Mesh(mesh.devices.reshape(NX, 2, NY, NZ), ("x", "core", "y", "z"))
    tok, voc = ("x", "core"), ("y", "z")
    in_specs = (P(tok, voc), P(tok, voc), P(tok))
    out_specs = (P(tok), P(tok, voc), P(tok, voc))
    return jax.shard_map(step, mesh=chips, in_specs=in_specs, out_specs=out_specs, check_vma=False)
```

```python
import functools

import jax
import jax.numpy as jnp
from jax import lax
from jax.experimental import pallas as pl
from jax.experimental.pallas import tpu as pltpu
from jax.sharding import Mesh, PartitionSpec as P


BF = jnp.bfloat16
F32 = jnp.float32
NX, NY, NZ = 4, 4, 8
STEPS = 4


def shift(a, axis, n, s):
    return lax.ppermute(a, axis, [(i, (i + s) % n) for i in range(n)])


def swap(a):
    return lax.ppermute(a, "core", [(0, 1), (1, 0)])


def from_everyone(a, axis, n):
    return lax.all_to_all(jnp.broadcast_to(a[None], (n, *a.shape)), axis, 0, 0, tiled=True)


def dot(a, b):
    return lax.dot_general(a, b, (((1,), (0,)), ((), ())), preferred_element_type=F32)


def whole(a):
    zeros = (0,) * a.ndim
    return pl.BlockSpec(a.shape, lambda j, s: zeros)


def early(j):
    return jnp.minimum(j, STEPS // 2 - 1)


def late(j):
    return jnp.maximum(j - STEPS // 2, 0)


def call(kernel, scalars, args, in_specs, out_specs, out_shape, flops, scratch=(), steps=STEPS):
    return pl.pallas_call(
        kernel,
        grid_spec=pltpu.PrefetchScalarGridSpec(
            num_scalar_prefetch=1,
            grid=(steps,),
            in_specs=in_specs,
            out_specs=out_specs,
            scratch_shapes=scratch,
        ),
        out_shape=out_shape,
        cost_estimate=pl.CostEstimate(flops=flops, bytes_accessed=flops // 256, transcendentals=0),
    )(jnp.stack(scalars).astype(jnp.int32), *args)


def prepare_kernel(who, p0, p1, p2, p3, digits, states, wanted):
    part = p0.shape[1]
    for j, parts in enumerate((p0, p1, p2, p3)):
        chip = (who[0] + j) % NY
        for c in range(2):
            rows = parts[4 * c : 4 * c + 4].reshape(4 * part, -1)
            states[2 * chip + c] = rows.T
            wanted[2 * chip + c, :part, :] = parts[4 * c + who[0]]
            wanted[2 * chip + c, part:, :] = digits[...]


def prepared(parts, digits, y):
    _, part, tokens = parts[0].shape
    states = jax.ShapeDtypeStruct((8, tokens, 4 * part), BF)
    wanted = jax.ShapeDtypeStruct((8, part + 16, tokens), BF)
    args = [*parts, digits]
    return call(
        prepare_kernel,
        [y, y],
        args,
        [whole(a) for a in args],
        [whole(states), whole(wanted)],
        [states, wanted],
        1 << 20,
        steps=1,
    )


def part_kernel(who, states, *refs, own, halves, more):
    *arrays, out = refs
    first = pl.program_id(0) < STEPS // 2

    def total(chosen, at):
        acc = arrays[-1][...] if more else None
        for k, ref in list(enumerate(arrays[:own])) + list(enumerate(chosen, at)):
            term = dot(states[who[k]], ref[...])
            acc = term if acc is None else acc + term
        out[...] = acc

    @pl.when(first)
    def _():
        total(arrays[own : own + halves], own)

    @pl.when(~first)
    def _():
        total(arrays[own + halves : own + 2 * halves], own + halves)


def logits_part(states, own, left, right, who, acc=None):
    rows, half = left[0].shape
    width = 2 * half
    tokens = states.shape[1]
    wide = width // STEPS
    tail = [] if acc is None else [acc]
    specs = [whole(states)] + [pl.BlockSpec((rows, wide), lambda j, s: (0, j))] * len(own)
    specs += [pl.BlockSpec((rows, wide), lambda j, s: (0, early(j)))] * len(left)
    specs += [pl.BlockSpec((rows, wide), lambda j, s: (0, late(j)))] * len(right)
    specs += [pl.BlockSpec((tokens, wide), lambda j, s: (0, j))] * len(tail)
    return call(
        functools.partial(part_kernel, own=len(own), halves=len(left), more=bool(tail)),
        who,
        [states, *own, *left, *right, *tail],
        specs,
        pl.BlockSpec((tokens, wide), lambda j, s: (0, j)),
        jax.ShapeDtypeStruct((tokens, width), F32),
        2 * (len(own) + len(left)) * tokens * rows * width,
    )


def far_kernel(who, mine_states, other_states, labels, near, left, left_other, right, right_other, powers, stats, logits):
    step = pl.program_id(0)
    first = step < STEPS // 2
    wide = near.shape[1]
    for mine, theirs, here in ((left, left_other, first), (right, right_other, ~first)):

        @pl.when(here)
        def _():
            logits[:, pl.ds(pl.multiple_of(step * wide, wide), wide)] = (
                near[...] + dot(mine_states[0], mine[...]) + dot(other_states[0], theirs[...])
            )

    @pl.when(step == STEPS - 1)
    def _():
        values = logits[...]
        peak = jnp.max(values, axis=1, keepdims=True)
        shifted = jnp.exp(values - peak)
        columns = who[2] + lax.broadcasted_iota(jnp.int32, values.shape, 1)
        hits = labels[...] == columns
        total = jnp.sum(shifted, axis=1, keepdims=True)
        target = jnp.sum(jnp.where(hits, values, 0.0), axis=1, keepdims=True)
        powers[...] = shifted.astype(BF)
        tokens = values.shape[0]
        lanes = lax.broadcasted_iota(jnp.int32, (tokens, 128), 1)
        both = jnp.where(lanes == 0, peak, jnp.where(lanes == 1, total, target))
        stats[...] = both.T[:8]


def far_logits(states, labels, near, left, right, who):
    tokens, width = near.shape
    wide = width // STEPS
    rows = left[0].shape[0]
    args = [states, states, labels, near, *left, *right]
    specs = [pl.BlockSpec((1, tokens, rows), lambda j, s, k=k: (s[k], 0, 0)) for k in (0, 1)]
    specs += [whole(labels), pl.BlockSpec((tokens, wide), lambda j, s: (0, j))]
    specs += [pl.BlockSpec((rows, wide), lambda j, s: (0, early(j)))] * 2
    specs += [pl.BlockSpec((rows, wide), lambda j, s: (0, late(j)))] * 2
    powers = jax.ShapeDtypeStruct((tokens, width), BF)
    stats = jax.ShapeDtypeStruct((8, 128), F32)
    return call(
        far_kernel,
        who,
        args,
        specs,
        [whole(powers), whole(stats)],
        [powers, stats],
        4 * tokens * rows * width,
        [pltpu.VMEM((tokens, width), F32)],
    )


def terms_kernel(starts, powers, labels, parts, stats, *refs):
    *arrays, out, rows_out, errors = refs
    step = pl.program_id(0)
    width, tokens = errors.shape

    @pl.when(step == 0)
    def _():
        peaks = parts[:, 0, :]
        peak = jnp.max(peaks, axis=0, keepdims=True)
        total = jnp.sum(parts[:, 1, :] * jnp.exp(peaks - peak), axis=0, keepdims=True)
        target = jnp.sum(parts[:, 2, :], axis=0, keepdims=True)
        scale = jnp.exp(stats[0:1, :] - peak) / total
        loss = jnp.log(total) + peak - target
        rows_out[...] = jnp.concatenate([scale, loss] + [scale] * 6, axis=0)
        columns = starts[8] + lax.broadcasted_iota(jnp.int32, (width, tokens), 0)
        hit = jnp.where(columns == labels[...], 1.0, 0.0)
        errors[...] = (powers[...].T.astype(F32) * scale - hit).astype(BF)

    half = width // 2
    own, left, right = arrays[:2], arrays[2:8], arrays[8:]
    lefts = jnp.concatenate([a[:, :half] for a in own] + [a[...] for a in left], axis=0)
    rights = jnp.concatenate([a[:, half:] for a in own] + [a[...] for a in right], axis=0)
    term = dot(lefts, errors[:half, :]) + dot(rights, errors[half:, :])
    rows = own[0].shape[0]
    for k in range(8):
        at = pl.ds(pl.multiple_of(starts[k] + step * rows, 32), rows)
        out[at, :] = term[k * rows : (k + 1) * rows].astype(BF)


def state_terms(powers, labels, parts, stats, own, left, right, starts, depth):
    tokens, width = powers.shape
    rows = own[0].shape[0] // STEPS
    args = [powers, labels, parts, stats, *own, *left, *right]
    specs = [whole(a) for a in args[:4]]
    specs += [pl.BlockSpec((rows, a.shape[1]), lambda j, s: (j, 0)) for a in args[4:]]
    terms = jax.ShapeDtypeStruct((depth, tokens), BF)
    rows_out = jax.ShapeDtypeStruct((8, tokens), F32)
    return call(
        terms_kernel,
        starts,
        args,
        specs,
        [whole(terms), whole(rows_out)],
        [terms, rows_out],
        2 * tokens * width * depth,
        [pltpu.VMEM((width, tokens), BF)],
    )


def grad_kernel(who, p0, p1, p2, p3, scales, *refs):
    *arrays, out, states, turned = refs
    step = pl.program_id(0)
    groups, padded, tokens = p0.shape
    part = padded - 16
    wide = out.shape[1]

    @pl.when(step == 0)
    def _():
        for j, parts in enumerate((p0, p1, p2, p3)):
            at = pl.multiple_of(((who[9] + j) % NY) * part, 32)
            for k in range(groups):
                states[k, pl.ds(at, part), :] = parts[k, :part, :]
        for k in range(groups):
            digits = p0[who[k], part:, :].astype(F32)
            number = digits[0:1] * 256.0 + digits[1:2]
            both = jnp.concatenate([number, scales[k : k + 1, :], digits[:6]], axis=0)
            turned[k] = both.T

    columns = who[8] + step * wide + lax.broadcasted_iota(jnp.int32, (tokens, wide), 1)
    columns = columns.astype(F32)
    blocks = [a[...] for a in arrays[:6]]
    first = step < STEPS // 2
    blocks += [jnp.where(first, arrays[6 + k][...], arrays[8 + k][...]) for k in range(2)]
    acc = None
    for pair in range(4):
        left, right = [], []
        for k in (2 * pair, 2 * pair + 1):
            hit = jnp.where(turned[k][:, 0:1] == columns, 1.0, 0.0)
            right.append((blocks[k].astype(F32) * turned[k][:, 1:2] - hit).astype(BF))
            left.append(states[who[k]])
        term = dot(jnp.concatenate(left, axis=1), jnp.concatenate(right, axis=0))
        acc = term if acc is None else acc + term
    out[...] = acc


def head_grad_of(parts, scales, near, left, right, who):
    groups, padded, tokens = parts[0].shape
    rows = NY * (padded - 16)
    width = near[0].shape[1]
    wide = width // STEPS
    args = [*parts, scales, *near, *left, *right]
    specs = [whole(a) for a in args[:5]]
    specs += [pl.BlockSpec((tokens, wide), lambda j, s: (0, j))] * 6
    specs += [pl.BlockSpec((tokens, wide), lambda j, s: (0, early(j)))] * 2
    specs += [pl.BlockSpec((tokens, wide), lambda j, s: (0, late(j)))] * 2
    return call(
        grad_kernel,
        who,
        args,
        specs,
        pl.BlockSpec((rows, wide), lambda j, s: (0, j)),
        jax.ShapeDtypeStruct((rows, width), F32),
        2 * groups * tokens * rows * width,
        [pltpu.VMEM((groups, rows, tokens), BF), pltpu.VMEM((groups, tokens, 8), F32)],
    )


def step(hidden_states, head, labels):
    x, core, y = lax.axis_index("x"), lax.axis_index("core"), lax.axis_index("y")
    vocab = y * NZ + lax.axis_index("z")
    tokens, part = hidden_states.shape
    rows, width = head.shape
    half = width // 2
    depth = NY * NZ * part
    base = vocab * width

    def who(offset):
        chip = ((x + offset) % NX) * 2
        return [chip + core, chip + 1 - core]

    up_left = shift(head[:, :half], "x", NX, 1)
    down_right = shift(head[:, half:], "x", NX, -1)
    up_right = shift(head[:, half:], "x", NX, 1)
    down_left = shift(head[:, :half], "x", NX, -1)
    own = [head, swap(head)]
    far_left = shift(up_left, "x", NX, 1)
    far_right = shift(down_right, "x", NX, -1)
    up_left_other, down_right_other = swap(up_left), swap(down_right)
    left = [down_left, swap(down_left)]
    right = [up_right, swap(up_right)]
    away_left = [far_left, swap(far_left)]
    away_right = [far_right, swap(far_right)]

    row = from_everyone(hidden_states.T, "z", NZ)
    parts = [row] + [shift(row, "y", NY, -j) for j in (1, 2, 3)]
    digits = jnp.stack([labels // 256, labels % 256]).astype(BF)
    digits = jnp.pad(digits, ((0, 14), (0, 0)))
    states, wanted = prepared(parts, digits, y)
    wanted = lax.all_to_all(wanted, ("x", "core"), 0, 0, tiled=True)
    far_states, wanted = lax.optimization_barrier((states, wanted))

    slices = [wanted] + [shift(wanted, "y", NY, -j) for j in (1, 2, 3)]
    logits = logits_part(
        states,
        own,
        [up_left, up_left_other],
        [down_right, down_right_other],
        who(0) + who(3) + who(1),
    )
    logits = logits_part(states, [], left, right, who(1) + who(3), logits)
    powers, stats = far_logits(
        far_states, labels[:, None], logits, away_left, away_right, who(2) + [base]
    )

    pow_up = shift(powers, "x", NX, 1)
    pow_down = shift(powers, "x", NX, -1)
    pow_left = shift(pow_up[:, :half], "x", NX, 1)
    pow_right = shift(pow_down[:, half:], "x", NX, -1)
    pow_near = [powers, swap(powers), pow_up, swap(pow_up), pow_down, swap(pow_down)]
    pow_left = [pow_left, swap(pow_left)]
    pow_right = [pow_right, swap(pow_right)]

    parts = from_everyone(stats[:3], ("y", "z"), NY * NZ)
    starts = [w * rows for w in who(0) + who(3) + who(1) + who(2)]
    all_left = [up_left, up_left_other, *left, *away_left]
    all_right = [*right, down_right, down_right_other, *away_right]
    terms, lines = state_terms(
        powers, labels[None], parts, stats, own, all_left, all_right, starts + [base], depth
    )
    scale, token_loss = lines[0], lines[1]

    arrived = lax.all_to_all(
        terms.reshape(NY * NZ, part, tokens), ("y", "z"), 0, 0, tiled=True
    )
    state_grad = arrived.astype(F32).sum(axis=0).astype(BF).T

    scale = jnp.stack([scale, swap(scale)])
    scales = [scale] + [shift(scale, "x", NX, s) for s in (1, -1, 2)]
    scales = jnp.concatenate(scales)
    head_grad = head_grad_of(
        slices,
        scales,
        pow_near,
        pow_left,
        pow_right,
        who(0) + who(3) + who(1) + who(2) + [base, y],
    )
    return (token_loss, state_grad, head_grad)


def solution(mesh):
    chips = Mesh(mesh.devices.reshape(NX, 2, NY, NZ), ("x", "core", "y", "z"))
    tok, voc = ("x", "core"), ("y", "z")
    in_specs = (P(tok, voc), P(tok, voc), P(tok))
    out_specs = (P(tok), P(tok, voc), P(tok, voc))
    return jax.shard_map(step, mesh=chips, in_specs=in_specs, out_specs=out_specs, check_vma=False)
```

```python
import functools

import jax
import jax.numpy as jnp
from jax import lax
from jax.experimental import pallas as pl
from jax.experimental.pallas import tpu as pltpu
from jax.sharding import Mesh, PartitionSpec as P


BF = jnp.bfloat16
F32 = jnp.float32
NX, NY, NZ = 4, 4, 8
STEPS = 2
ROOM = 65000 << 10


def shift(a, axis, n, s):
    return lax.ppermute(a, axis, [(i, (i + s) % n) for i in range(n)])


def swap(a):
    return lax.ppermute(a, "core", [(0, 1), (1, 0)])


def from_everyone(a, axis, n):
    return lax.all_to_all(jnp.broadcast_to(a[None], (n, *a.shape)), axis, 0, 0, tiled=True)


def dot(a, b):
    return lax.dot_general(a, b, (((1,), (0,)), ((), ())), preferred_element_type=F32)


def whole(a):
    zeros = (0,) * a.ndim
    return pl.BlockSpec(a.shape, lambda j, s: zeros)


def early(j):
    return jnp.minimum(j, STEPS // 2 - 1)


def late(j):
    return jnp.maximum(j - STEPS // 2, 0)


def call(kernel, scalars, args, in_specs, out_specs, out_shape, flops, scratch=(), steps=STEPS, room=None):
    return pl.pallas_call(
        kernel,
        grid_spec=pltpu.PrefetchScalarGridSpec(
            num_scalar_prefetch=1,
            grid=(steps,),
            in_specs=in_specs,
            out_specs=out_specs,
            scratch_shapes=scratch,
        ),
        out_shape=out_shape,
        compiler_params=pltpu.CompilerParams(vmem_limit_bytes=room),
        cost_estimate=pl.CostEstimate(flops=flops, bytes_accessed=flops // 256, transcendentals=0),
    )(jnp.stack(scalars).astype(jnp.int32), *args)


def prepare_kernel(who, p0, p1, p2, p3, digits, states, wanted):
    part = p0.shape[1]
    for j, parts in enumerate((p0, p1, p2, p3)):
        chip = (who[0] + j) % NY
        for c in range(2):
            rows = parts[4 * c : 4 * c + 4].reshape(4 * part, -1)
            states[2 * chip + c] = rows.T
            wanted[2 * chip + c, :part, :] = parts[4 * c + who[0]]
            wanted[2 * chip + c, part:, :] = digits[...]


def prepared(parts, digits, y):
    _, part, tokens = parts[0].shape
    states = jax.ShapeDtypeStruct((8, tokens, 4 * part), BF)
    wanted = jax.ShapeDtypeStruct((8, part + 16, tokens), BF)
    args = [*parts, digits]
    return call(
        prepare_kernel,
        [y, y],
        args,
        [whole(a) for a in args],
        [whole(states), whole(wanted)],
        [states, wanted],
        1 << 20,
        steps=1,
    )


def part_kernel(who, states, *refs, own, halves, more):
    *arrays, out = refs
    first = pl.program_id(0) < STEPS // 2

    def total(chosen, at):
        acc = arrays[-1][...] if more else None
        for k, ref in list(enumerate(arrays[:own])) + list(enumerate(chosen, at)):
            term = dot(states[who[k]], ref[...])
            acc = term if acc is None else acc + term
        out[...] = acc

    @pl.when(first)
    def _():
        total(arrays[own : own + halves], own)

    @pl.when(~first)
    def _():
        total(arrays[own + halves : own + 2 * halves], own + halves)


def logits_part(states, own, left, right, who, acc=None):
    rows, half = left[0].shape
    width = 2 * half
    tokens = states.shape[1]
    wide = width // STEPS
    tail = [] if acc is None else [acc]
    specs = [whole(states)] + [pl.BlockSpec((rows, wide), lambda j, s: (0, j))] * len(own)
    specs += [pl.BlockSpec((rows, wide), lambda j, s: (0, early(j)))] * len(left)
    specs += [pl.BlockSpec((rows, wide), lambda j, s: (0, late(j)))] * len(right)
    specs += [pl.BlockSpec((tokens, wide), lambda j, s: (0, j))] * len(tail)
    return call(
        functools.partial(part_kernel, own=len(own), halves=len(left), more=bool(tail)),
        who,
        [states, *own, *left, *right, *tail],
        specs,
        pl.BlockSpec((tokens, wide), lambda j, s: (0, j)),
        jax.ShapeDtypeStruct((tokens, width), F32),
        2 * (len(own) + len(left)) * tokens * rows * width,
    )


def far_kernel(who, states, labels, near, left, left_other, right, right_other, powers, stats, logits, rows, few, sems):
    copies = [
        pltpu.make_async_copy(states.at[who[0]], few.at[0], sems.at[0]),
        pltpu.make_async_copy(states.at[who[1]], few.at[1], sems.at[1]),
        pltpu.make_async_copy(left, rows.at[0], sems.at[2]),
        pltpu.make_async_copy(left_other, rows.at[1], sems.at[3]),
        pltpu.make_async_copy(near, logits, sems.at[4]),
        pltpu.make_async_copy(right, rows.at[2], sems.at[5]),
        pltpu.make_async_copy(right_other, rows.at[3], sems.at[6]),
    ]
    for copy in copies:
        copy.start()
    half = rows.shape[2]
    for side, ready in ((0, copies[:5]), (1, copies[5:])):
        for copy in ready:
            copy.wait()
        at = slice(side * half, (side + 1) * half)
        logits[:, at] += dot(few[0], rows[2 * side]) + dot(few[1], rows[2 * side + 1])
    values = logits[...]
    peak = jnp.max(values, axis=1, keepdims=True)
    shifted = jnp.exp(values - peak)
    columns = who[2] + lax.broadcasted_iota(jnp.int32, values.shape, 1)
    hits = labels[...] == columns
    total = jnp.sum(shifted, axis=1, keepdims=True)
    target = jnp.sum(jnp.where(hits, values, 0.0), axis=1, keepdims=True)
    powers[...] = shifted.astype(BF)
    lanes = lax.broadcasted_iota(jnp.int32, (values.shape[0], 128), 1)
    both = jnp.where(lanes == 0, peak, jnp.where(lanes == 1, total, target))
    stats[...] = both.T[:8]


def far_logits(states, labels, near, left, right, who):
    tokens, width = near.shape
    rows, half = left[0].shape
    args = [states, labels, near, *left, *right]
    far = pl.BlockSpec(memory_space=pltpu.HBM)
    powers = jax.ShapeDtypeStruct((tokens, width), BF)
    stats = jax.ShapeDtypeStruct((8, 128), F32)
    return call(
        far_kernel,
        who,
        args,
        [far, whole(labels)] + [far] * 5,
        [whole(powers), whole(stats)],
        [powers, stats],
        4 * tokens * rows * width,
        [
            pltpu.VMEM((tokens, width), F32),
            pltpu.VMEM((4, rows, half), BF),
            pltpu.VMEM((2, tokens, rows), BF),
            pltpu.SemaphoreType.DMA((7,)),
        ],
        steps=1,
        room=ROOM,
    )


def terms_kernel(starts, powers, labels, parts, stats, *refs):
    *arrays, out, scales, losses, errors = refs
    step = pl.program_id(0)
    width, tokens = errors.shape

    @pl.when(step == 0)
    def _():
        peaks = parts[:, 0, :]
        peak = jnp.max(peaks, axis=0, keepdims=True)
        total = jnp.sum(parts[:, 1, :] * jnp.exp(peaks - peak), axis=0, keepdims=True)
        target = jnp.sum(parts[:, 2, :], axis=0, keepdims=True)
        scale = jnp.exp(stats[0:1, :] - peak) / total
        loss = jnp.log(total) + peak - target
        scales[...] = scale
        losses[...] = loss
        columns = starts[8] + lax.broadcasted_iota(jnp.int32, (width, tokens), 0)
        hit = jnp.where(columns == labels[...], 1.0, 0.0)
        errors[...] = (powers[...].T.astype(F32) * scale - hit).astype(BF)

    half = width // 2
    own, left, right = arrays[:2], arrays[2:8], arrays[8:]
    lefts = jnp.concatenate([a[:, :half] for a in own] + [a[...] for a in left], axis=0)
    rights = jnp.concatenate([a[:, half:] for a in own] + [a[...] for a in right], axis=0)
    term = dot(lefts, errors[:half, :]) + dot(rights, errors[half:, :])
    rows = own[0].shape[0]
    for k in range(8):
        at = pl.ds(pl.multiple_of(starts[k] + step * rows, 32), rows)
        out[at, :] = term[k * rows : (k + 1) * rows].astype(BF)


def state_terms(powers, labels, parts, stats, own, left, right, starts, depth):
    tokens, width = powers.shape
    rows = own[0].shape[0] // STEPS
    args = [powers, labels, parts, stats, *own, *left, *right]
    specs = [whole(a) for a in args[:4]]
    specs += [pl.BlockSpec((rows, a.shape[1]), lambda j, s: (j, 0)) for a in args[4:]]
    terms = jax.ShapeDtypeStruct((depth, tokens), BF)
    line = jax.ShapeDtypeStruct((1, tokens), F32)
    return call(
        terms_kernel,
        starts,
        args,
        specs,
        [whole(terms), whole(line), whole(line)],
        [terms, line, line],
        2 * tokens * width * depth,
        [pltpu.VMEM((width, tokens), BF)],
    )


def grad_kernel(who, p0, p1, p2, p3, *refs):
    *arrays, out, states, turned = refs
    scales, arrays = arrays[:4], arrays[4:]
    step = pl.program_id(0)
    groups, padded, tokens = p0.shape
    part = padded - 16
    wide = out.shape[1]

    @pl.when(step == 0)
    def _():
        for j, parts in enumerate((p0, p1, p2, p3)):
            at = pl.multiple_of(((who[9] + j) % NY) * part, 32)
            for k in range(groups):
                states[k, pl.ds(at, part), :] = parts[k, :part, :]
        for k in range(groups):
            digits = p0[who[k], part:, :].astype(F32)
            number = digits[0:1] * 256.0 + digits[1:2]
            scale = scales[k // 2][k % 2 : k % 2 + 1, :]
            both = jnp.concatenate([number, scale, digits[:6]], axis=0)
            turned[k] = both.T

    columns = who[8] + step * wide + lax.broadcasted_iota(jnp.int32, (tokens, wide), 1)
    columns = columns.astype(F32)
    blocks = [a[...] for a in arrays[:6]]
    first = step < STEPS // 2
    blocks += [jnp.where(first, arrays[6 + k][...], arrays[8 + k][...]) for k in range(2)]
    acc = None
    for pair in range(4):
        left, right = [], []
        for k in (2 * pair, 2 * pair + 1):
            hit = jnp.where(turned[k][:, 0:1] == columns, 1.0, 0.0)
            right.append((blocks[k].astype(F32) * turned[k][:, 1:2] - hit).astype(BF))
            left.append(states[who[k]])
        term = dot(jnp.concatenate(left, axis=1), jnp.concatenate(right, axis=0))
        acc = term if acc is None else acc + term
    out[...] = acc


def head_grad_of(parts, scales, near, left, right, who):
    groups, padded, tokens = parts[0].shape
    rows = NY * (padded - 16)
    width = near[0].shape[1]
    wide = width // STEPS
    args = [*parts, *scales, *near, *left, *right]
    specs = [whole(a) for a in args[:8]]
    specs += [pl.BlockSpec((tokens, wide), lambda j, s: (0, j))] * 6
    specs += [pl.BlockSpec((tokens, wide), lambda j, s: (0, early(j)))] * 2
    specs += [pl.BlockSpec((tokens, wide), lambda j, s: (0, late(j)))] * 2
    return call(
        grad_kernel,
        who,
        args,
        specs,
        pl.BlockSpec((rows, wide), lambda j, s: (0, j)),
        jax.ShapeDtypeStruct((rows, width), F32),
        2 * groups * tokens * rows * width,
        [pltpu.VMEM((groups, rows, tokens), BF), pltpu.VMEM((groups, tokens, 8), F32)],
    )


def step(hidden_states, head, labels):
    x, core, y = lax.axis_index("x"), lax.axis_index("core"), lax.axis_index("y")
    vocab = y * NZ + lax.axis_index("z")
    tokens, part = hidden_states.shape
    rows, width = head.shape
    half = width // 2
    depth = NY * NZ * part
    base = vocab * width

    def who(offset):
        chip = ((x + offset) % NX) * 2
        return [chip + core, chip + 1 - core]

    left_half = head[:, :half]
    right_half = lax.optimization_barrier(head)[:, half:]
    up_left = shift(left_half, "x", NX, 1)
    down_right = shift(right_half, "x", NX, -1)
    up_right = shift(right_half, "x", NX, 1)
    down_left = shift(left_half, "x", NX, -1)
    own = [head, swap(head)]
    far_left = shift(up_left, "x", NX, 1)
    far_right = shift(down_right, "x", NX, -1)
    up_left_other, down_right_other = swap(up_left), swap(down_right)
    left = [down_left, swap(down_left)]
    right = [up_right, swap(up_right)]
    away_left = [far_left, swap(far_left)]
    away_right = [far_right, swap(far_right)]

    row = from_everyone(hidden_states.T, "z", NZ)
    parts = [row] + [shift(row, "y", NY, -j) for j in (1, 2, 3)]
    digits = jnp.stack([labels // 256, labels % 256]).astype(BF)
    digits = jnp.pad(digits, ((0, 14), (0, 0)))
    states, wanted = prepared(parts, digits, y)
    wanted = lax.all_to_all(wanted, ("x", "core"), 0, 0, tiled=True)
    far_states, wanted = lax.optimization_barrier((states, wanted))

    slices = [wanted] + [shift(wanted, "y", NY, -j) for j in (1, 2, 3)]
    logits = logits_part(
        states,
        own,
        [up_left, up_left_other],
        [down_right, down_right_other],
        who(0) + who(3) + who(1),
    )
    logits = logits_part(states, [], left, right, who(1) + who(3), logits)
    powers, stats = far_logits(
        far_states, labels[:, None], logits, away_left, away_right, who(2) + [base]
    )

    pow_up = shift(powers, "x", NX, 1)
    pow_down = shift(powers, "x", NX, -1)
    pow_left = shift(pow_up[:, :half], "x", NX, 1)
    pow_right = shift(pow_down[:, half:], "x", NX, -1)
    pow_near = [powers, swap(powers), pow_up, swap(pow_up), pow_down, swap(pow_down)]
    pow_left = [pow_left, swap(pow_left)]
    pow_right = [pow_right, swap(pow_right)]

    parts = from_everyone(stats[:3], ("y", "z"), NY * NZ)
    starts = [w * rows for w in who(0) + who(3) + who(1) + who(2)]
    all_left = [up_left, up_left_other, *left, *away_left]
    all_right = [*right, down_right, down_right_other, *away_right]
    terms, scale, token_loss = state_terms(
        powers, labels[None], parts, stats, own, all_left, all_right, starts + [base], depth
    )
    token_loss = token_loss.reshape(tokens)

    arrived = lax.all_to_all(
        terms.reshape(NY * NZ, part, tokens), ("y", "z"), 0, 0, tiled=True
    )
    state_grad = arrived.astype(F32).sum(axis=0).astype(BF).T

    pair = jnp.concatenate([scale, swap(scale)])
    scales = [pair] + [shift(pair, "x", NX, s) for s in (1, -1, 2)]
    head_grad = head_grad_of(
        slices,
        scales,
        pow_near,
        pow_left,
        pow_right,
        who(0) + who(3) + who(1) + who(2) + [base, y],
    )
    return (token_loss, state_grad, head_grad)


def solution(mesh):
    chips = Mesh(mesh.devices.reshape(NX, 2, NY, NZ), ("x", "core", "y", "z"))
    tok, voc = ("x", "core"), ("y", "z")
    in_specs = (P(tok, voc), P(tok, voc), P(tok))
    out_specs = (P(tok), P(tok, voc), P(tok, voc))
    return jax.shard_map(step, mesh=chips, in_specs=in_specs, out_specs=out_specs, check_vma=False)
```

```python
import functools

import jax
import jax.numpy as jnp
from jax import lax
from jax.experimental import pallas as pl
from jax.experimental.pallas import tpu as pltpu
from jax.sharding import Mesh, PartitionSpec as P


BF = jnp.bfloat16
F32 = jnp.float32
NX, NY, NZ = 4, 4, 8
STEPS = 2
ROOM = 65000 << 10


def shift(a, axis, n, s):
    return lax.ppermute(a, axis, [(i, (i + s) % n) for i in range(n)])


def swap(a):
    return lax.ppermute(a, "core", [(0, 1), (1, 0)])


def from_everyone(a, axis, n):
    return lax.all_to_all(jnp.broadcast_to(a[None], (n, *a.shape)), axis, 0, 0, tiled=True)


def dot(a, b):
    return lax.dot_general(a, b, (((1,), (0,)), ((), ())), preferred_element_type=F32)


def whole(a):
    zeros = (0,) * a.ndim
    return pl.BlockSpec(a.shape, lambda j, s: zeros)


def early(j):
    return jnp.minimum(j, STEPS // 2 - 1)


def late(j):
    return jnp.maximum(j - STEPS // 2, 0)


def call(kernel, scalars, args, in_specs, out_specs, out_shape, flops, scratch=(), steps=STEPS, room=ROOM):
    return pl.pallas_call(
        kernel,
        grid_spec=pltpu.PrefetchScalarGridSpec(
            num_scalar_prefetch=1,
            grid=(steps,),
            in_specs=in_specs,
            out_specs=out_specs,
            scratch_shapes=scratch,
        ),
        out_shape=out_shape,
        compiler_params=pltpu.CompilerParams(vmem_limit_bytes=room),
        cost_estimate=pl.CostEstimate(flops=flops, bytes_accessed=flops // 256, transcendentals=0),
    )(jnp.stack(scalars).astype(jnp.int32), *args)


def prepare_kernel(who, p0, p1, p2, p3, digits, states, wanted):
    part = p0.shape[1]
    for j, parts in enumerate((p0, p1, p2, p3)):
        chip = (who[0] + j) % NY
        for c in range(2):
            rows = parts[4 * c : 4 * c + 4].reshape(4 * part, -1)
            states[2 * chip + c] = rows.T
            wanted[2 * chip + c, :part, :] = parts[4 * c + who[0]]
            wanted[2 * chip + c, part:, :] = digits[...]


def prepared(parts, digits, y):
    _, part, tokens = parts[0].shape
    states = jax.ShapeDtypeStruct((8, tokens, 4 * part), BF)
    wanted = jax.ShapeDtypeStruct((8, part + 16, tokens), BF)
    args = [*parts, digits]
    return call(
        prepare_kernel,
        [y, y],
        args,
        [whole(a) for a in args],
        [whole(states), whole(wanted)],
        [states, wanted],
        1 << 20,
        steps=1,
    )


def part_kernel(who, states, *refs, own, halves, more):
    *arrays, out = refs
    first = pl.program_id(0) < STEPS // 2

    def total(chosen, at):
        acc = arrays[-1][...] if more else None
        for k, ref in list(enumerate(arrays[:own])) + list(enumerate(chosen, at)):
            term = dot(states[who[k]], ref[...])
            acc = term if acc is None else acc + term
        out[...] = acc

    @pl.when(first)
    def _():
        total(arrays[own : own + halves], own)

    @pl.when(~first)
    def _():
        total(arrays[own + halves : own + 2 * halves], own + halves)


def logits_part(states, own, left, right, who, acc=None):
    rows, half = left[0].shape
    width = 2 * half
    tokens = states.shape[1]
    wide = width // STEPS
    tail = [] if acc is None else [acc]
    specs = [whole(states)] + [pl.BlockSpec((rows, wide), lambda j, s: (0, j))] * len(own)
    specs += [pl.BlockSpec((rows, wide), lambda j, s: (0, early(j)))] * len(left)
    specs += [pl.BlockSpec((rows, wide), lambda j, s: (0, late(j)))] * len(right)
    specs += [pl.BlockSpec((tokens, wide), lambda j, s: (0, j))] * len(tail)
    return call(
        functools.partial(part_kernel, own=len(own), halves=len(left), more=bool(tail)),
        who,
        [states, *own, *left, *right, *tail],
        specs,
        pl.BlockSpec((tokens, wide), lambda j, s: (0, j)),
        jax.ShapeDtypeStruct((tokens, width), F32),
        2 * (len(own) + len(left)) * tokens * rows * width,
    )


def far_kernel(who, states, labels, near, left, left_other, right, right_other, powers, stats, peaks, logits, rows, few, sems):
    copies = [
        pltpu.make_async_copy(states.at[who[0]], few.at[0], sems.at[0]),
        pltpu.make_async_copy(states.at[who[1]], few.at[1], sems.at[1]),
        pltpu.make_async_copy(left, rows.at[0], sems.at[2]),
        pltpu.make_async_copy(left_other, rows.at[1], sems.at[3]),
        pltpu.make_async_copy(near, logits, sems.at[4]),
        pltpu.make_async_copy(right, rows.at[2], sems.at[5]),
        pltpu.make_async_copy(right_other, rows.at[3], sems.at[6]),
    ]
    for copy in copies:
        copy.start()
    half = rows.shape[2]
    for side, ready in ((0, copies[:5]), (1, copies[5:])):
        for copy in ready:
            copy.wait()
        at = slice(side * half, (side + 1) * half)
        logits[:, at] += dot(few[0], rows[2 * side]) + dot(few[1], rows[2 * side + 1])
    values = logits[...]
    peak = jnp.max(values, axis=1, keepdims=True)
    shifted = jnp.exp(values - peak)
    columns = who[2] + lax.broadcasted_iota(jnp.int32, values.shape, 1)
    hits = labels[...] == columns
    total = jnp.sum(shifted, axis=1, keepdims=True)
    target = jnp.sum(jnp.where(hits, values, 0.0), axis=1, keepdims=True)
    powers[...] = shifted.astype(BF)
    lanes = lax.broadcasted_iota(jnp.int32, (values.shape[0], 128), 1)
    both = jnp.where(lanes == 0, peak, jnp.where(lanes == 1, total, target))
    lines = both.T
    stats[...] = jnp.broadcast_to(lines[None, :3], stats.shape)
    peaks[...] = lines[:1]


def far_logits(states, labels, near, left, right, who):
    tokens, width = near.shape
    rows, half = left[0].shape
    args = [states, labels, near, *left, *right]
    far = pl.BlockSpec(memory_space=pltpu.HBM)
    powers = jax.ShapeDtypeStruct((tokens, width), BF)
    stats = jax.ShapeDtypeStruct((NY * NZ, 3, tokens), F32)
    peaks = jax.ShapeDtypeStruct((1, tokens), F32)
    return call(
        far_kernel,
        who,
        args,
        [far, whole(labels)] + [far] * 5,
        [whole(powers), whole(stats), whole(peaks)],
        [powers, stats, peaks],
        4 * tokens * rows * width,
        [
            pltpu.VMEM((tokens, width), F32),
            pltpu.VMEM((4, rows, half), BF),
            pltpu.VMEM((2, tokens, rows), BF),
            pltpu.SemaphoreType.DMA((7,)),
        ],
        steps=1,
        room=ROOM,
    )


def terms_kernel(starts, powers, labels, parts, peaks, *refs):
    *arrays, out0, out1, out2, out3, scales, losses, errors, out = refs
    step = pl.program_id(0)
    width, tokens = errors.shape

    @pl.when(step == 0)
    def _():
        theirs = parts[:, 0, :]
        peak = jnp.max(theirs, axis=0, keepdims=True)
        total = jnp.sum(parts[:, 1, :] * jnp.exp(theirs - peak), axis=0, keepdims=True)
        target = jnp.sum(parts[:, 2, :], axis=0, keepdims=True)
        scale = jnp.exp(peaks[...] - peak) / total
        loss = jnp.log(total) + peak - target
        scales[...] = scale
        losses[...] = loss
        columns = starts[8] + lax.broadcasted_iota(jnp.int32, (width, tokens), 0)
        hit = jnp.where(columns == labels[...], 1.0, 0.0)
        errors[...] = (powers[...].T.astype(F32) * scale - hit).astype(BF)

    half = width // 2
    own, left, right = arrays[:2], arrays[2:8], arrays[8:]
    lefts = jnp.concatenate([a[:, :half] for a in own] + [a[...] for a in left], axis=0)
    rights = jnp.concatenate([a[:, half:] for a in own] + [a[...] for a in right], axis=0)
    term = dot(lefts, errors[:half, :]) + dot(rights, errors[half:, :])
    rows = own[0].shape[0]
    for k in range(8):
        at = pl.ds(pl.multiple_of(starts[k] + step * rows, 32), rows)
        out[at, :] = term[k * rows : (k + 1) * rows].astype(BF)

    @pl.when(step == STEPS - 1)
    def _():
        for j, ref in enumerate((out0, out1, out2, out3)):
            ref[...] = out[pl.ds(j * ref.shape[0], ref.shape[0]), :]


def state_terms(powers, labels, parts, peaks, own, left, right, starts, depth):
    tokens, width = powers.shape
    rows = own[0].shape[0] // STEPS
    args = [powers, labels, parts, peaks, *own, *left, *right]
    specs = [whole(a) for a in args[:4]]
    specs += [pl.BlockSpec((rows, a.shape[1]), lambda j, s: (j, 0)) for a in args[4:]]
    terms = jax.ShapeDtypeStruct((depth // NY, tokens), BF)
    line = jax.ShapeDtypeStruct((1, tokens), F32)
    return call(
        terms_kernel,
        starts,
        args,
        specs,
        [whole(terms)] * NY + [whole(line)] * 2,
        [terms] * NY + [line] * 2,
        2 * tokens * width * depth,
        [pltpu.VMEM((width, tokens), BF), pltpu.VMEM((depth, tokens), BF)],
    )


def grad_kernel(who, p0, p1, p2, p3, *refs):
    *arrays, out, states, turned = refs
    scales, arrays = arrays[:4], arrays[4:]
    step = pl.program_id(0)
    groups, padded, tokens = p0.shape
    part = padded - 16
    wide = out.shape[1]

    @pl.when(step == 0)
    def _():
        for j, parts in enumerate((p0, p1, p2, p3)):
            at = pl.multiple_of(((who[9] + j) % NY) * part, 32)
            for k in range(groups):
                states[k, pl.ds(at, part), :] = parts[k, :part, :]
        for k in range(groups):
            digits = p0[who[k], part:, :].astype(F32)
            number = digits[0:1] * 256.0 + digits[1:2]
            scale = scales[k // 2][k % 2 : k % 2 + 1, :]
            both = jnp.concatenate([number, scale, digits[:6]], axis=0)
            turned[k] = both.T

    columns = who[8] + step * wide + lax.broadcasted_iota(jnp.int32, (tokens, wide), 1)
    columns = columns.astype(F32)
    blocks = [a[...] for a in arrays[:6]]
    first = step < STEPS // 2
    blocks += [jnp.where(first, arrays[6 + k][...], arrays[8 + k][...]) for k in range(2)]
    acc = None
    for pair in range(4):
        left, right = [], []
        for k in (2 * pair, 2 * pair + 1):
            hit = jnp.where(turned[k][:, 0:1] == columns, 1.0, 0.0)
            right.append((blocks[k].astype(F32) * turned[k][:, 1:2] - hit).astype(BF))
            left.append(states[who[k]])
        term = dot(jnp.concatenate(left, axis=1), jnp.concatenate(right, axis=0))
        acc = term if acc is None else acc + term
    out[...] = acc


def head_grad_of(parts, scales, near, left, right, who):
    groups, padded, tokens = parts[0].shape
    rows = NY * (padded - 16)
    width = near[0].shape[1]
    wide = width // STEPS
    args = [*parts, *scales, *near, *left, *right]
    specs = [whole(a) for a in args[:8]]
    specs += [pl.BlockSpec((tokens, wide), lambda j, s: (0, j))] * 6
    specs += [pl.BlockSpec((tokens, wide), lambda j, s: (0, early(j)))] * 2
    specs += [pl.BlockSpec((tokens, wide), lambda j, s: (0, late(j)))] * 2
    return call(
        grad_kernel,
        who,
        args,
        specs,
        pl.BlockSpec((rows, wide), lambda j, s: (0, j)),
        jax.ShapeDtypeStruct((rows, width), F32),
        2 * groups * tokens * rows * width,
        [pltpu.VMEM((groups, rows, tokens), BF), pltpu.VMEM((groups, tokens, 8), F32)],
    )


def step(hidden_states, head, labels):
    x, core, y = lax.axis_index("x"), lax.axis_index("core"), lax.axis_index("y")
    vocab = y * NZ + lax.axis_index("z")
    tokens, part = hidden_states.shape
    rows, width = head.shape
    half = width // 2
    depth = NY * NZ * part
    base = vocab * width

    def who(offset):
        chip = ((x + offset) % NX) * 2
        return [chip + core, chip + 1 - core]

    left_half = head[:, :half]
    right_half = lax.optimization_barrier(head)[:, half:]
    up_left = shift(left_half, "x", NX, 1)
    down_right = shift(right_half, "x", NX, -1)
    up_right = shift(right_half, "x", NX, 1)
    down_left = shift(left_half, "x", NX, -1)
    own = [head, swap(head)]
    far_left = shift(up_left, "x", NX, 1)
    far_right = shift(down_right, "x", NX, -1)
    up_left_other, down_right_other = swap(up_left), swap(down_right)
    left = [down_left, swap(down_left)]
    right = [up_right, swap(up_right)]
    away_left = [far_left, swap(far_left)]
    away_right = [far_right, swap(far_right)]

    row = from_everyone(hidden_states.T, "z", NZ)
    parts = [row] + [shift(row, "y", NY, -j) for j in (1, 2, 3)]
    digits = jnp.stack([labels // 256, labels % 256]).astype(BF)
    digits = jnp.pad(digits, ((0, 14), (0, 0)))
    states, wanted = prepared(parts, digits, y)
    wanted = lax.all_to_all(wanted, ("x", "core"), 0, 0, tiled=True)
    far_states, wanted = lax.optimization_barrier((states, wanted))

    slices = [wanted] + [shift(wanted, "y", NY, -j) for j in (1, 2, 3)]
    logits = logits_part(
        states,
        own,
        [up_left, up_left_other],
        [down_right, down_right_other],
        who(0) + who(3) + who(1),
    )
    logits = logits_part(states, [], left, right, who(1) + who(3), logits)
    powers, stats, peaks = far_logits(
        far_states, labels[:, None], logits, away_left, away_right, who(2) + [base]
    )

    pow_up = shift(powers, "x", NX, 1)
    pow_down = shift(powers, "x", NX, -1)
    pow_left = shift(pow_up[:, :half], "x", NX, 1)
    pow_right = shift(pow_down[:, half:], "x", NX, -1)
    pow_near = [powers, swap(powers), pow_up, swap(pow_up), pow_down, swap(pow_down)]
    pow_left = [pow_left, swap(pow_left)]
    pow_right = [pow_right, swap(pow_right)]

    parts = lax.all_to_all(stats, ("y", "z"), 0, 0, tiled=True)
    starts = []
    for offset in (0, 3, 1, 2):
        chip = ((x + offset - y) % NY) * 2
        starts += [(chip + core) * rows, (chip + 1 - core) * rows]
    all_left = [up_left, up_left_other, *left, *away_left]
    all_right = [*right, down_right, down_right_other, *away_right]
    *terms, scale, token_loss = state_terms(
        powers, labels[None], parts, peaks, own, all_left, all_right, starts + [base], depth
    )
    token_loss = token_loss.reshape(tokens)

    arrived = [terms[0]] + [shift(terms[j], "y", NY, j) for j in (1, 2, 3)]
    row_sum = sum(a.astype(F32) for a in arrived).astype(BF)
    arrived = lax.all_to_all(row_sum.reshape(NZ, part, tokens), "z", 0, 0, tiled=True)
    state_grad = arrived.astype(F32).sum(axis=0).astype(BF).T

    pair = jnp.concatenate([scale, swap(scale)])
    scales = [pair] + [shift(pair, "x", NX, s) for s in (1, -1, 2)]
    head_grad = head_grad_of(
        slices,
        scales,
        pow_near,
        pow_left,
        pow_right,
        who(0) + who(3) + who(1) + who(2) + [base, y],
    )
    return (token_loss, state_grad, head_grad)


def solution(mesh):
    chips = Mesh(mesh.devices.reshape(NX, 2, NY, NZ), ("x", "core", "y", "z"))
    tok, voc = ("x", "core"), ("y", "z")
    in_specs = (P(tok, voc), P(tok, voc), P(tok))
    out_specs = (P(tok), P(tok, voc), P(tok, voc))
    return jax.shard_map(step, mesh=chips, in_specs=in_specs, out_specs=out_specs, check_vma=False)
```

```python
import functools

import jax
import jax.numpy as jnp
from jax import lax
from jax.experimental import pallas as pl
from jax.experimental.pallas import tpu as pltpu
from jax.sharding import Mesh, PartitionSpec as P


BF = jnp.bfloat16
F32 = jnp.float32
NX, NY, NZ = 4, 4, 8
STEPS = 2
ROOM = 65000 << 10


def shift(a, axis, n, s):
    return lax.ppermute(a, axis, [(i, (i + s) % n) for i in range(n)])


def swap(a):
    return lax.ppermute(a, "core", [(0, 1), (1, 0)])


def from_everyone(a, axis, n):
    return lax.all_to_all(jnp.broadcast_to(a[None], (n, *a.shape)), axis, 0, 0, tiled=True)


def dot(a, b):
    return lax.dot_general(a, b, (((1,), (0,)), ((), ())), preferred_element_type=F32)


def whole(a):
    zeros = (0,) * a.ndim
    return pl.BlockSpec(a.shape, lambda j, s: zeros)


def early(j):
    return jnp.minimum(j, STEPS // 2 - 1)


def late(j):
    return jnp.maximum(j - STEPS // 2, 0)


def call(kernel, scalars, args, in_specs, out_specs, out_shape, flops, scratch=(), steps=STEPS, room=None):
    return pl.pallas_call(
        kernel,
        grid_spec=pltpu.PrefetchScalarGridSpec(
            num_scalar_prefetch=1,
            grid=(steps,),
            in_specs=in_specs,
            out_specs=out_specs,
            scratch_shapes=scratch,
        ),
        out_shape=out_shape,
        compiler_params=pltpu.CompilerParams(vmem_limit_bytes=room),
        cost_estimate=pl.CostEstimate(flops=flops, bytes_accessed=flops // 256, transcendentals=0),
    )(jnp.stack(scalars).astype(jnp.int32), *args)


def prepare_kernel(who, p0, p1, p2, p3, digits, states, wanted):
    part = p0.shape[1]
    for j, parts in enumerate((p0, p1, p2, p3)):
        chip = (who[0] + j) % NY
        for c in range(2):
            rows = parts[4 * c : 4 * c + 4].reshape(4 * part, -1)
            states[2 * chip + c] = rows.T
            wanted[2 * chip + c, :part, :] = parts[4 * c + who[0]]
            wanted[2 * chip + c, part:, :] = digits[...]


def prepared(parts, digits, y):
    _, part, tokens = parts[0].shape
    states = jax.ShapeDtypeStruct((8, tokens, 4 * part), BF)
    wanted = jax.ShapeDtypeStruct((8, part + 16, tokens), BF)
    args = [*parts, digits]
    return call(
        prepare_kernel,
        [y, y],
        args,
        [whole(a) for a in args],
        [whole(states), whole(wanted)],
        [states, wanted],
        1 << 20,
        steps=1,
    )


def part_kernel(who, states, *refs, own, halves, more):
    *arrays, out = refs
    first = pl.program_id(0) < STEPS // 2

    def total(chosen, at):
        acc = arrays[-1][...] if more else None
        for k, ref in list(enumerate(arrays[:own])) + list(enumerate(chosen, at)):
            term = dot(states[who[k]], ref[...])
            acc = term if acc is None else acc + term
        out[...] = acc

    @pl.when(first)
    def _():
        total(arrays[own : own + halves], own)

    @pl.when(~first)
    def _():
        total(arrays[own + halves : own + 2 * halves], own + halves)


def logits_part(states, own, left, right, who, acc=None):
    rows, half = left[0].shape
    width = 2 * half
    tokens = states.shape[1]
    wide = width // STEPS
    tail = [] if acc is None else [acc]
    specs = [whole(states)] + [pl.BlockSpec((rows, wide), lambda j, s: (0, j))] * len(own)
    specs += [pl.BlockSpec((rows, wide), lambda j, s: (0, early(j)))] * len(left)
    specs += [pl.BlockSpec((rows, wide), lambda j, s: (0, late(j)))] * len(right)
    specs += [pl.BlockSpec((tokens, wide), lambda j, s: (0, j))] * len(tail)
    return call(
        functools.partial(part_kernel, own=len(own), halves=len(left), more=bool(tail)),
        who,
        [states, *own, *left, *right, *tail],
        specs,
        pl.BlockSpec((tokens, wide), lambda j, s: (0, j)),
        jax.ShapeDtypeStruct((tokens, width), F32),
        2 * (len(own) + len(left)) * tokens * rows * width,
    )


def far_kernel(who, states, labels, near, left, left_other, right, right_other, powers, stats, peaks, logits, rows, few, sems):
    depth = states.shape[2]
    wide = rows.shape[2]
    per = left.shape[1] // wide
    copies = [
        pltpu.make_async_copy(states.at[who[k]], few.at[:, k * depth : (k + 1) * depth], sems.at[k])
        for k in (0, 1)
    ]
    ready = []
    for q in range(2 * per):
        mine, theirs = ((left, left_other), (right, right_other))[q // per]
        at = slice((q % per) * wide, (q % per + 1) * wide)
        ready.append(
            [
                pltpu.make_async_copy(mine.at[:, at], rows.at[q, :depth], sems.at[2 + 3 * q]),
                pltpu.make_async_copy(theirs.at[:, at], rows.at[q, depth:], sems.at[3 + 3 * q]),
                pltpu.make_async_copy(
                    near.at[:, q * wide : (q + 1) * wide],
                    logits.at[:, q * wide : (q + 1) * wide],
                    sems.at[4 + 3 * q],
                ),
            ]
        )
        copies += ready[-1]
    for copy in copies:
        copy.start()
    for copy in copies[:2]:
        copy.wait()
    for q in range(2 * per):
        for copy in ready[q]:
            copy.wait()
        logits[:, q * wide : (q + 1) * wide] += dot(few[...], rows[q])
    values = logits[...]
    peak = jnp.max(values, axis=1, keepdims=True)
    shifted = jnp.exp(values - peak)
    columns = who[2] + lax.broadcasted_iota(jnp.int32, values.shape, 1)
    hits = labels[...] == columns
    total = jnp.sum(shifted, axis=1, keepdims=True)
    target = jnp.sum(jnp.where(hits, values, 0.0), axis=1, keepdims=True)
    powers[...] = shifted.astype(BF)
    lanes = lax.broadcasted_iota(jnp.int32, (values.shape[0], 128), 1)
    lines = jnp.where(lanes == 0, peak, jnp.where(lanes == 1, total, target)).T
    stats[...] = jnp.broadcast_to(lines[None, :3], stats.shape)
    peaks[...] = lines[:1]


def far_logits(states, labels, near, left, right, who, wide=512):
    tokens, width = near.shape
    rows, _ = left[0].shape
    args = [states, labels, near, *left, *right]
    far = pl.BlockSpec(memory_space=pltpu.HBM)
    powers = jax.ShapeDtypeStruct((tokens, width), BF)
    stats = jax.ShapeDtypeStruct((NY * NZ, 3, tokens), F32)
    peaks = jax.ShapeDtypeStruct((1, tokens), F32)
    count = width // wide
    return call(
        far_kernel,
        who,
        args,
        [far, whole(labels)] + [far] * 5,
        [whole(powers), whole(stats), whole(peaks)],
        [powers, stats, peaks],
        4 * tokens * rows * width,
        [
            pltpu.VMEM((tokens, width), F32),
            pltpu.VMEM((count, 2 * rows, wide), BF),
            pltpu.VMEM((tokens, 2 * rows), BF),
            pltpu.SemaphoreType.DMA((2 + 3 * count,)),
        ],
        steps=1,
        room=ROOM,
    )


def terms_kernel(starts, powers, labels, parts, peaks, *refs):
    arrays, (out, scales, losses, errors, full, cut, pieces, sems, done) = refs[:14], refs[14:]
    width, tokens = errors.shape
    half = width // 2
    rows = cut.shape[1]

    loads = [[pltpu.make_async_copy(arrays[k], full.at[k], sems.at[k])] for k in range(2)]
    loads += [
        [pltpu.make_async_copy(arrays[j + k], cut.at[j - 2 + k], sems.at[j + k]) for j in (2, 8)]
        for k in range(6)
    ]
    for load in loads:
        for copy in load:
            copy.start()

    theirs = parts[:, 0, :]
    peak = jnp.max(theirs, axis=0, keepdims=True)
    total = jnp.sum(parts[:, 1, :] * jnp.exp(theirs - peak), axis=0, keepdims=True)
    target = jnp.sum(parts[:, 2, :], axis=0, keepdims=True)
    scale = jnp.exp(peaks[...] - peak) / total
    scales[...] = scale
    losses[...] = jnp.log(total) + peak - target
    columns = starts[8] + lax.broadcasted_iota(jnp.int32, (width, tokens), 0)
    hit = jnp.where(columns == labels[...], 1.0, 0.0)
    errors[...] = (powers[...].T.astype(F32) * scale - hit).astype(BF)

    stores = []
    for k in range(8):
        for copy in loads[k]:
            copy.wait()
        if k < 2:
            term = dot(full[k], errors[...])
        else:
            term = dot(cut[k - 2], errors[:half, :]) + dot(cut[k + 4], errors[half:, :])
        pieces[k] = term.astype(BF)
        at = pl.ds(pl.multiple_of(starts[k], rows), rows)
        stores.append(pltpu.make_async_copy(pieces.at[k], out.at[at], done.at[k]))
        stores[-1].start()
    for copy in stores:
        copy.wait()


def state_terms(powers, labels, parts, peaks, own, left, right, starts, depth):
    tokens, width = powers.shape
    rows = own[0].shape[0]
    args = [powers, labels, parts, peaks, *own, *left, *right]
    away = pl.BlockSpec(memory_space=pltpu.HBM)
    terms = jax.ShapeDtypeStruct((depth, tokens), BF)
    line = jax.ShapeDtypeStruct((1, tokens), F32)
    return call(
        terms_kernel,
        starts,
        args,
        [whole(a) for a in args[:4]] + [away] * 14,
        [away, whole(line), whole(line)],
        [terms, line, line],
        2 * tokens * width * depth,
        [
            pltpu.VMEM((width, tokens), BF),
            pltpu.VMEM((2, rows, width), BF),
            pltpu.VMEM((12, rows, width // 2), BF),
            pltpu.VMEM((8, rows, tokens), BF),
            pltpu.SemaphoreType.DMA((14,)),
            pltpu.SemaphoreType.DMA((8,)),
        ],
        steps=1,
        room=ROOM,
    )


def grad_kernel(who, p0, p1, p2, p3, *refs):
    *arrays, out, states, turned = refs
    scales, arrays = arrays[:4], arrays[4:]
    step = pl.program_id(0)
    groups, padded, tokens = p0.shape
    part = padded - 16
    wide = out.shape[1]

    @pl.when(step == 0)
    def _():
        for j, parts in enumerate((p0, p1, p2, p3)):
            at = pl.multiple_of(((who[9] + j) % NY) * part, 32)
            for k in range(groups):
                states[k, pl.ds(at, part), :] = parts[k, :part, :]
        for k in range(groups):
            digits = p0[who[k], part:, :].astype(F32)
            number = digits[0:1] * 256.0 + digits[1:2]
            scale = scales[k // 2][k % 2 : k % 2 + 1, :]
            both = jnp.concatenate([number, scale, digits[:6]], axis=0)
            turned[k] = both.T

    columns = who[8] + step * wide + lax.broadcasted_iota(jnp.int32, (tokens, wide), 1)
    columns = columns.astype(F32)
    blocks = [a[...] for a in arrays]
    acc = None
    for pair in range(4):
        left, right = [], []
        for k in (2 * pair, 2 * pair + 1):
            hit = jnp.where(turned[k][:, 0:1] == columns, 1.0, 0.0)
            right.append((blocks[k].astype(F32) * turned[k][:, 1:2] - hit).astype(BF))
            left.append(states[who[k]])
        term = dot(jnp.concatenate(left, axis=1), jnp.concatenate(right, axis=0))
        acc = term if acc is None else acc + term
    out[...] = acc


def head_grad_of(parts, scales, blocks, who):
    groups, padded, tokens = parts[0].shape
    rows = NY * (padded - 16)
    width = blocks[0].shape[1]
    wide = width // STEPS
    args = [*parts, *scales, *blocks]
    specs = [whole(a) for a in args[:8]]
    specs += [pl.BlockSpec((tokens, wide), lambda j, s: (0, j))] * 8
    return call(
        grad_kernel,
        who,
        args,
        specs,
        pl.BlockSpec((rows, wide), lambda j, s: (0, j)),
        jax.ShapeDtypeStruct((rows, width), F32),
        2 * groups * tokens * rows * width,
        [pltpu.VMEM((groups, rows, tokens), BF), pltpu.VMEM((groups, tokens, 8), F32)],
    )


def step(hidden_states, head, labels):
    x, core, y = lax.axis_index("x"), lax.axis_index("core"), lax.axis_index("y")
    vocab = y * NZ + lax.axis_index("z")
    tokens, part = hidden_states.shape
    rows, width = head.shape
    half = width // 2
    depth = NY * NZ * part
    base = vocab * width

    def who(offset):
        chip = ((x + offset) % NX) * 2
        return [chip + core, chip + 1 - core]

    left_half = head[:, :half]
    right_half = lax.optimization_barrier(head)[:, half:]
    up_left = shift(left_half, "x", NX, 1)
    down_right = shift(right_half, "x", NX, -1)
    up_right = shift(right_half, "x", NX, 1)
    down_left = shift(left_half, "x", NX, -1)
    own = [head, swap(head)]
    far_left = shift(up_left, "x", NX, 1)
    far_right = shift(down_right, "x", NX, -1)
    up_left_other, down_right_other = swap(up_left), swap(down_right)
    left = [down_left, swap(down_left)]
    right = [up_right, swap(up_right)]
    away_left = [far_left, swap(far_left)]
    away_right = [far_right, swap(far_right)]

    row = from_everyone(hidden_states.T, "z", NZ)
    parts = [row] + [shift(row, "y", NY, -j) for j in (1, 2, 3)]
    digits = jnp.stack([labels // 256, labels % 256]).astype(BF)
    digits = jnp.pad(digits, ((0, 14), (0, 0)))
    states, wanted = prepared(parts, digits, y)
    wanted = lax.all_to_all(wanted, ("x", "core"), 0, 0, tiled=True)
    far_states, wanted = lax.optimization_barrier((states, wanted))

    slices = [wanted] + [shift(wanted, "y", NY, -j) for j in (1, 2, 3)]
    logits = logits_part(
        states,
        own,
        [up_left, up_left_other],
        [down_right, down_right_other],
        who(0) + who(3) + who(1),
    )
    logits = logits_part(states, [], left, right, who(1) + who(3), logits)
    powers, stats, peaks = far_logits(
        far_states, labels[:, None], logits, away_left, away_right, who(2) + [base]
    )

    pow_up = shift(powers, "x", NX, 1)
    pow_down = shift(powers, "x", NX, -1)
    pow_far = shift(powers, "x", NX, 2)
    pow_own = swap(powers)
    blocks = [powers, pow_own]
    for block in (pow_up, pow_down, pow_far):
        blocks += [block, swap(block)]

    parts = lax.all_to_all(stats, ("y", "z"), 0, 0, tiled=True)
    starts = [w * rows for w in who(0) + who(3) + who(1) + who(2)]
    all_left = [up_left, up_left_other, *left, *away_left]
    all_right = [*right, down_right, down_right_other, *away_right]
    terms, scale, token_loss = state_terms(
        powers, labels[None], parts, peaks, own, all_left, all_right, starts + [base], depth
    )
    token_loss = token_loss.reshape(tokens)

    arrived = lax.all_to_all(
        terms.reshape(NY * NZ, part, tokens), ("y", "z"), 0, 0, tiled=True
    )
    state_grad = arrived.astype(F32).sum(axis=0).astype(BF).T

    pair = jnp.concatenate([scale, swap(scale)])
    scales = [pair] + [shift(pair, "x", NX, s) for s in (1, -1, 2)]
    head_grad = head_grad_of(slices, scales, blocks, who(0) + who(3) + who(1) + who(2) + [base, y])
    return (token_loss, state_grad, head_grad)


def solution(mesh):
    chips = Mesh(mesh.devices.reshape(NX, 2, NY, NZ), ("x", "core", "y", "z"))
    tok, voc = ("x", "core"), ("y", "z")
    in_specs = (P(tok, voc), P(tok, voc), P(tok))
    out_specs = (P(tok), P(tok, voc), P(tok, voc))
    return jax.shard_map(step, mesh=chips, in_specs=in_specs, out_specs=out_specs, check_vma=False)
```

```python
import functools

import jax
import jax.numpy as jnp
from jax import lax
from jax.experimental import pallas as pl
from jax.experimental.pallas import tpu as pltpu
from jax.sharding import Mesh, PartitionSpec as P


BF = jnp.bfloat16
F32 = jnp.float32
NX, NY, NZ = 4, 4, 8
STEPS = 2
ROOM = 65000 << 10


def shift(a, axis, n, s):
    return lax.ppermute(a, axis, [(i, (i + s) % n) for i in range(n)])


def swap(a):
    return lax.ppermute(a, "core", [(0, 1), (1, 0)])


def from_everyone(a, axis, n):
    return lax.all_to_all(jnp.broadcast_to(a[None], (n, *a.shape)), axis, 0, 0, tiled=True)


def dot(a, b):
    return lax.dot_general(a, b, (((1,), (0,)), ((), ())), preferred_element_type=F32)


def whole(a):
    zeros = (0,) * a.ndim
    return pl.BlockSpec(a.shape, lambda j, s: zeros)


def early(j):
    return jnp.minimum(j, STEPS // 2 - 1)


def late(j):
    return jnp.maximum(j - STEPS // 2, 0)


def call(kernel, scalars, args, in_specs, out_specs, out_shape, flops, scratch=(), steps=STEPS, room=None):
    return pl.pallas_call(
        kernel,
        grid_spec=pltpu.PrefetchScalarGridSpec(
            num_scalar_prefetch=1,
            grid=(steps,),
            in_specs=in_specs,
            out_specs=out_specs,
            scratch_shapes=scratch,
        ),
        out_shape=out_shape,
        compiler_params=pltpu.CompilerParams(vmem_limit_bytes=room),
        cost_estimate=pl.CostEstimate(flops=flops, bytes_accessed=flops // 256, transcendentals=0),
    )(jnp.stack(scalars).astype(jnp.int32), *args)


def prepare_kernel(who, p0, p1, p2, p3, digits, states, wanted):
    part = p0.shape[1]
    for j, parts in enumerate((p0, p1, p2, p3)):
        chip = (who[0] + j) % NY
        for c in range(2):
            rows = parts[4 * c : 4 * c + 4].reshape(4 * part, -1)
            states[2 * chip + c] = rows.T
            wanted[2 * chip + c, :part, :] = parts[4 * c + who[0]]
            wanted[2 * chip + c, part:, :] = digits[...]


def prepared(parts, digits, y):
    _, part, tokens = parts[0].shape
    states = jax.ShapeDtypeStruct((8, tokens, 4 * part), BF)
    wanted = jax.ShapeDtypeStruct((8, part + 16, tokens), BF)
    args = [*parts, digits]
    return call(
        prepare_kernel,
        [y, y],
        args,
        [whole(a) for a in args],
        [whole(states), whole(wanted)],
        [states, wanted],
        1 << 20,
        steps=1,
    )


def part_kernel(who, states, *refs, own, halves, more):
    *arrays, out = refs
    first = pl.program_id(0) < STEPS // 2

    def total(chosen, at):
        acc = arrays[-1][...] if more else None
        for k, ref in list(enumerate(arrays[:own])) + list(enumerate(chosen, at)):
            term = dot(states[who[k]], ref[...])
            acc = term if acc is None else acc + term
        out[...] = acc

    @pl.when(first)
    def _():
        total(arrays[own : own + halves], own)

    @pl.when(~first)
    def _():
        total(arrays[own + halves : own + 2 * halves], own + halves)


def logits_part(states, own, left, right, who, acc=None):
    rows, half = left[0].shape
    width = 2 * half
    tokens = states.shape[1]
    wide = width // STEPS
    tail = [] if acc is None else [acc]
    specs = [whole(states)] + [pl.BlockSpec((rows, wide), lambda j, s: (0, j))] * len(own)
    specs += [pl.BlockSpec((rows, wide), lambda j, s: (0, early(j)))] * len(left)
    specs += [pl.BlockSpec((rows, wide), lambda j, s: (0, late(j)))] * len(right)
    specs += [pl.BlockSpec((tokens, wide), lambda j, s: (0, j))] * len(tail)
    return call(
        functools.partial(part_kernel, own=len(own), halves=len(left), more=bool(tail)),
        who,
        [states, *own, *left, *right, *tail],
        specs,
        pl.BlockSpec((tokens, wide), lambda j, s: (0, j)),
        jax.ShapeDtypeStruct((tokens, width), F32),
        2 * (len(own) + len(left)) * tokens * rows * width,
    )


def far_kernel(who, states, labels, near, left, left_other, right, right_other, powers, stats, peaks, logits, rows, few, sems):
    depth = states.shape[2]
    wide = rows.shape[2]
    per = left.shape[1] // wide
    copies = [
        pltpu.make_async_copy(states.at[who[k]], few.at[:, k * depth : (k + 1) * depth], sems.at[k])
        for k in (0, 1)
    ]
    ready = []
    for q in range(2 * per):
        mine, theirs = ((left, left_other), (right, right_other))[q // per]
        at = slice((q % per) * wide, (q % per + 1) * wide)
        ready.append(
            [
                pltpu.make_async_copy(mine.at[:, at], rows.at[q, :depth], sems.at[2 + 3 * q]),
                pltpu.make_async_copy(theirs.at[:, at], rows.at[q, depth:], sems.at[3 + 3 * q]),
                pltpu.make_async_copy(
                    near.at[:, q * wide : (q + 1) * wide],
                    logits.at[:, q * wide : (q + 1) * wide],
                    sems.at[4 + 3 * q],
                ),
            ]
        )
        copies += ready[-1]
    for copy in copies:
        copy.start()
    for copy in copies[:2]:
        copy.wait()
    for q in range(2 * per):
        for copy in ready[q]:
            copy.wait()
        logits[:, q * wide : (q + 1) * wide] += dot(few[...], rows[q])
    values = logits[...]
    peak = jnp.max(values, axis=1, keepdims=True)
    shifted = jnp.exp(values - peak)
    columns = who[2] + lax.broadcasted_iota(jnp.int32, values.shape, 1)
    hits = labels[...] == columns
    total = jnp.sum(shifted, axis=1, keepdims=True)
    target = jnp.sum(jnp.where(hits, values, 0.0), axis=1, keepdims=True)
    powers[...] = shifted.astype(BF)
    lanes = lax.broadcasted_iota(jnp.int32, (values.shape[0], 128), 1)
    lines = jnp.where(lanes == 0, peak, jnp.where(lanes == 1, total, target)).T
    stats[...] = jnp.broadcast_to(lines[None, :3], stats.shape)
    peaks[...] = lines[:1]


def far_logits(states, labels, near, left, right, who, wide=512):
    tokens, width = near.shape
    rows, _ = left[0].shape
    args = [states, labels, near, *left, *right]
    far = pl.BlockSpec(memory_space=pltpu.HBM)
    powers = jax.ShapeDtypeStruct((tokens, width), BF)
    stats = jax.ShapeDtypeStruct((NY * NZ, 3, tokens), F32)
    peaks = jax.ShapeDtypeStruct((1, tokens), F32)
    count = width // wide
    return call(
        far_kernel,
        who,
        args,
        [far, whole(labels)] + [far] * 5,
        [whole(powers), whole(stats), whole(peaks)],
        [powers, stats, peaks],
        4 * tokens * rows * width,
        [
            pltpu.VMEM((tokens, width), F32),
            pltpu.VMEM((count, 2 * rows, wide), BF),
            pltpu.VMEM((tokens, 2 * rows), BF),
            pltpu.SemaphoreType.DMA((2 + 3 * count,)),
        ],
        steps=1,
        room=ROOM,
    )


def terms_kernel(starts, powers, labels, parts, peaks, *refs):
    *arrays, out, scales, losses, errors = refs
    step = pl.program_id(0)
    width, tokens = errors.shape

    @pl.when(step == 0)
    def _():
        theirs = parts[:, 0, :]
        peak = jnp.max(theirs, axis=0, keepdims=True)
        total = jnp.sum(parts[:, 1, :] * jnp.exp(theirs - peak), axis=0, keepdims=True)
        target = jnp.sum(parts[:, 2, :], axis=0, keepdims=True)
        scale = jnp.exp(peaks[...] - peak) / total
        loss = jnp.log(total) + peak - target
        scales[...] = scale
        losses[...] = loss
        columns = starts[8] + lax.broadcasted_iota(jnp.int32, (width, tokens), 0)
        hit = jnp.where(columns == labels[...], 1.0, 0.0)
        errors[...] = (powers[...].T.astype(F32) * scale - hit).astype(BF)

    half = width // 2
    own, left, right = arrays[:2], arrays[2:8], arrays[8:]
    lefts = jnp.concatenate([a[:, :half] for a in own] + [a[...] for a in left], axis=0)
    rights = jnp.concatenate([a[:, half:] for a in own] + [a[...] for a in right], axis=0)
    term = dot(lefts, errors[:half, :]) + dot(rights, errors[half:, :])
    rows = own[0].shape[0]
    for k in range(8):
        at = pl.ds(pl.multiple_of(starts[k] + step * rows, 32), rows)
        out[at, :] = term[k * rows : (k + 1) * rows].astype(BF)


def state_terms(powers, labels, parts, peaks, own, left, right, starts, depth):
    tokens, width = powers.shape
    rows = own[0].shape[0] // STEPS
    args = [powers, labels, parts, peaks, *own, *left, *right]
    specs = [whole(a) for a in args[:4]]
    specs += [pl.BlockSpec((rows, a.shape[1]), lambda j, s: (j, 0)) for a in args[4:]]
    terms = jax.ShapeDtypeStruct((depth, tokens), BF)
    line = jax.ShapeDtypeStruct((1, tokens), F32)
    return call(
        terms_kernel,
        starts,
        args,
        specs,
        [whole(terms), whole(line), whole(line)],
        [terms, line, line],
        2 * tokens * width * depth,
        [pltpu.VMEM((width, tokens), BF)],
    )


def grad_kernel(who, p0, p1, p2, p3, *refs):
    *arrays, out, states, turned = refs
    scales, arrays = arrays[:4], arrays[4:]
    step = pl.program_id(0)
    groups, padded, tokens = p0.shape
    part = padded - 16
    wide = out.shape[1]

    @pl.when(step == 0)
    def _():
        for j, parts in enumerate((p0, p1, p2, p3)):
            at = pl.multiple_of(((who[9] + j) % NY) * part, 32)
            for k in range(groups):
                states[k, pl.ds(at, part), :] = parts[k, :part, :]
        for k in range(groups):
            digits = p0[who[k], part:, :].astype(F32)
            number = digits[0:1] * 256.0 + digits[1:2]
            scale = scales[k // 2][k % 2 : k % 2 + 1, :]
            both = jnp.concatenate([number, scale, digits[:6]], axis=0)
            turned[k] = both.T

    columns = who[8] + step * wide + lax.broadcasted_iota(jnp.int32, (tokens, wide), 1)
    columns = columns.astype(F32)
    blocks = [a[...] for a in arrays]
    acc = None
    for pair in range(4):
        left, right = [], []
        for k in (2 * pair, 2 * pair + 1):
            hit = jnp.where(turned[k][:, 0:1] == columns, 1.0, 0.0)
            right.append((blocks[k].astype(F32) * turned[k][:, 1:2] - hit).astype(BF))
            left.append(states[who[k]])
        term = dot(jnp.concatenate(left, axis=1), jnp.concatenate(right, axis=0))
        acc = term if acc is None else acc + term
    out[...] = acc


def head_grad_of(parts, scales, blocks, who):
    groups, padded, tokens = parts[0].shape
    rows = NY * (padded - 16)
    width = blocks[0].shape[1]
    wide = width // STEPS
    args = [*parts, *scales, *blocks]
    specs = [whole(a) for a in args[:8]]
    specs += [pl.BlockSpec((tokens, wide), lambda j, s: (0, j))] * 8
    return call(
        grad_kernel,
        who,
        args,
        specs,
        pl.BlockSpec((rows, wide), lambda j, s: (0, j)),
        jax.ShapeDtypeStruct((rows, width), F32),
        2 * groups * tokens * rows * width,
        [pltpu.VMEM((groups, rows, tokens), BF), pltpu.VMEM((groups, tokens, 8), F32)],
    )


def step(hidden_states, head, labels):
    x, core, y = lax.axis_index("x"), lax.axis_index("core"), lax.axis_index("y")
    vocab = y * NZ + lax.axis_index("z")
    tokens, part = hidden_states.shape
    rows, width = head.shape
    half = width // 2
    depth = NY * NZ * part
    base = vocab * width

    def who(offset):
        chip = ((x + offset) % NX) * 2
        return [chip + core, chip + 1 - core]

    left_half = head[:, :half]
    right_half = lax.optimization_barrier(head)[:, half:]
    up_left = shift(left_half, "x", NX, 1)
    down_right = shift(right_half, "x", NX, -1)
    up_right = shift(right_half, "x", NX, 1)
    down_left = shift(left_half, "x", NX, -1)
    own = [head, swap(head)]
    far_left = shift(up_left, "x", NX, 1)
    far_right = shift(down_right, "x", NX, -1)
    up_left_other, down_right_other = swap(up_left), swap(down_right)
    left = [down_left, swap(down_left)]
    right = [up_right, swap(up_right)]
    away_left = [far_left, swap(far_left)]
    away_right = [far_right, swap(far_right)]

    row = from_everyone(hidden_states.T, "z", NZ)
    parts = [row] + [shift(row, "y", NY, -j) for j in (1, 2, 3)]
    digits = jnp.stack([labels // 256, labels % 256]).astype(BF)
    digits = jnp.pad(digits, ((0, 14), (0, 0)))
    states, wanted = prepared(parts, digits, y)
    wanted = lax.all_to_all(wanted, ("x", "core"), 0, 0, tiled=True)
    far_states, wanted = lax.optimization_barrier((states, wanted))

    slices = [wanted] + [shift(wanted, "y", NY, -j) for j in (1, 2, 3)]
    logits = logits_part(
        states,
        own,
        [up_left, up_left_other],
        [down_right, down_right_other],
        who(0) + who(3) + who(1),
    )
    logits = logits_part(states, [], left, right, who(1) + who(3), logits)
    powers, stats, peaks = far_logits(
        far_states, labels[:, None], logits, away_left, away_right, who(2) + [base]
    )

    pow_up = shift(powers, "x", NX, 1)
    pow_down = shift(powers, "x", NX, -1)
    pow_far = shift(powers, "x", NX, 2)
    pow_own = swap(powers)
    blocks = [powers, pow_own]
    for block in (pow_up, pow_down, pow_far):
        blocks += [block, swap(block)]

    parts = lax.all_to_all(stats, ("y", "z"), 0, 0, tiled=True)
    starts = [w * rows for w in who(0) + who(3) + who(1) + who(2)]
    all_left = [up_left, up_left_other, *left, *away_left]
    all_right = [*right, down_right, down_right_other, *away_right]
    terms, scale, token_loss = state_terms(
        powers, labels[None], parts, peaks, own, all_left, all_right, starts + [base], depth
    )
    token_loss = token_loss.reshape(tokens)

    arrived = lax.all_to_all(
        terms.reshape(NY * NZ, part, tokens), ("y", "z"), 0, 0, tiled=True
    )
    state_grad = arrived.astype(F32).sum(axis=0).astype(BF).T

    pair = jnp.concatenate([scale, swap(scale)])
    scales = [pair] + [shift(pair, "x", NX, s) for s in (1, -1, 2)]
    head_grad = head_grad_of(slices, scales, blocks, who(0) + who(3) + who(1) + who(2) + [base, y])
    return (token_loss, state_grad, head_grad)


def solution(mesh):
    chips = Mesh(mesh.devices.reshape(NX, 2, NY, NZ), ("x", "core", "y", "z"))
    tok, voc = ("x", "core"), ("y", "z")
    in_specs = (P(tok, voc), P(tok, voc), P(tok))
    out_specs = (P(tok), P(tok, voc), P(tok, voc))
    return jax.shard_map(step, mesh=chips, in_specs=in_specs, out_specs=out_specs, check_vma=False)
```

```python
import functools

import jax
import jax.numpy as jnp
from jax import lax
from jax.experimental import pallas as pl
from jax.experimental.pallas import tpu as pltpu
from jax.sharding import Mesh, PartitionSpec as P


BF = jnp.bfloat16
F32 = jnp.float32
NX, NY, NZ = 4, 4, 8
STEPS = 2
ROOM = 65000 << 10


def shift(a, axis, n, s):
    return lax.ppermute(a, axis, [(i, (i + s) % n) for i in range(n)])


def swap(a):
    return lax.ppermute(a, "core", [(0, 1), (1, 0)])


def from_everyone(a, axis, n):
    return lax.all_to_all(jnp.broadcast_to(a[None], (n, *a.shape)), axis, 0, 0, tiled=True)


def dot(a, b):
    return lax.dot_general(a, b, (((1,), (0,)), ((), ())), preferred_element_type=F32)


def whole(a):
    zeros = (0,) * a.ndim
    return pl.BlockSpec(a.shape, lambda j, s: zeros)


def early(j):
    return jnp.minimum(j, STEPS // 2 - 1)


def late(j):
    return jnp.maximum(j - STEPS // 2, 0)


def call(kernel, scalars, args, in_specs, out_specs, out_shape, flops, scratch=(), steps=STEPS, room=None):
    return pl.pallas_call(
        kernel,
        grid_spec=pltpu.PrefetchScalarGridSpec(
            num_scalar_prefetch=1,
            grid=(steps,),
            in_specs=in_specs,
            out_specs=out_specs,
            scratch_shapes=scratch,
        ),
        out_shape=out_shape,
        compiler_params=pltpu.CompilerParams(vmem_limit_bytes=room),
        cost_estimate=pl.CostEstimate(flops=flops, bytes_accessed=flops // 256, transcendentals=0),
    )(jnp.stack(scalars).astype(jnp.int32), *args)


def prepare_kernel(who, p0, p1, p2, p3, digits, states, wanted):
    part = p0.shape[1]
    for j, parts in enumerate((p0, p1, p2, p3)):
        chip = (who[0] + j) % NY
        for c in range(2):
            rows = parts[4 * c : 4 * c + 4].reshape(4 * part, -1)
            states[2 * chip + c] = rows.T
            wanted[2 * chip + c, :part, :] = parts[4 * c + who[0]]
            wanted[2 * chip + c, part:, :] = digits[...]


def prepared(parts, digits, y):
    _, part, tokens = parts[0].shape
    states = jax.ShapeDtypeStruct((8, tokens, 4 * part), BF)
    wanted = jax.ShapeDtypeStruct((8, part + 16, tokens), BF)
    args = [*parts, digits]
    return call(
        prepare_kernel,
        [y, y],
        args,
        [whole(a) for a in args],
        [whole(states), whole(wanted)],
        [states, wanted],
        1 << 20,
        steps=1,
    )


def part_kernel(who, states, *refs, own, halves, more):
    *arrays, out = refs
    first = pl.program_id(0) < STEPS // 2

    def total(chosen, at):
        acc = arrays[-1][...] if more else None
        for k, ref in list(enumerate(arrays[:own])) + list(enumerate(chosen, at)):
            term = dot(states[who[k]], ref[...])
            acc = term if acc is None else acc + term
        out[...] = acc

    @pl.when(first)
    def _():
        total(arrays[own : own + halves], own)

    @pl.when(~first)
    def _():
        total(arrays[own + halves : own + 2 * halves], own + halves)


def logits_part(states, own, left, right, who, acc=None):
    rows, half = left[0].shape
    width = 2 * half
    tokens = states.shape[1]
    wide = width // STEPS
    tail = [] if acc is None else [acc]
    specs = [whole(states)] + [pl.BlockSpec((rows, wide), lambda j, s: (0, j))] * len(own)
    specs += [pl.BlockSpec((rows, wide), lambda j, s: (0, early(j)))] * len(left)
    specs += [pl.BlockSpec((rows, wide), lambda j, s: (0, late(j)))] * len(right)
    specs += [pl.BlockSpec((tokens, wide), lambda j, s: (0, j))] * len(tail)
    return call(
        functools.partial(part_kernel, own=len(own), halves=len(left), more=bool(tail)),
        who,
        [states, *own, *left, *right, *tail],
        specs,
        pl.BlockSpec((tokens, wide), lambda j, s: (0, j)),
        jax.ShapeDtypeStruct((tokens, width), F32),
        2 * (len(own) + len(left)) * tokens * rows * width,
    )


def far_kernel(who, states, labels, near, left, left_other, right, right_other, powers, stats, peaks, logits, rows, few, sems):
    depth = states.shape[2]
    wide = rows.shape[2]
    per = left.shape[1] // wide
    copies = [
        pltpu.make_async_copy(states.at[who[k]], few.at[:, k * depth : (k + 1) * depth], sems.at[k])
        for k in (0, 1)
    ]
    ready = []
    for q in range(2 * per):
        mine, theirs = ((left, left_other), (right, right_other))[q // per]
        at = slice((q % per) * wide, (q % per + 1) * wide)
        ready.append(
            [
                pltpu.make_async_copy(mine.at[:, at], rows.at[q, :depth], sems.at[2 + 3 * q]),
                pltpu.make_async_copy(theirs.at[:, at], rows.at[q, depth:], sems.at[3 + 3 * q]),
                pltpu.make_async_copy(
                    near.at[:, q * wide : (q + 1) * wide],
                    logits.at[:, q * wide : (q + 1) * wide],
                    sems.at[4 + 3 * q],
                ),
            ]
        )
        copies += ready[-1]
    for copy in copies:
        copy.start()
    for copy in copies[:2]:
        copy.wait()
    for q in range(2 * per):
        for copy in ready[q]:
            copy.wait()
        logits[:, q * wide : (q + 1) * wide] += dot(few[...], rows[q])
    values = logits[...]
    peak = jnp.max(values, axis=1, keepdims=True)
    shifted = jnp.exp(values - peak)
    columns = who[2] + lax.broadcasted_iota(jnp.int32, values.shape, 1)
    hits = labels[...] == columns
    total = jnp.sum(shifted, axis=1, keepdims=True)
    target = jnp.sum(jnp.where(hits, values, 0.0), axis=1, keepdims=True)
    powers[...] = shifted.astype(BF)
    lanes = lax.broadcasted_iota(jnp.int32, (values.shape[0], 128), 1)
    lines = jnp.where(lanes == 0, peak, jnp.where(lanes == 1, total, target)).T
    stats[...] = jnp.broadcast_to(lines[None, :3], stats.shape)
    peaks[...] = lines[:1]


def far_logits(states, labels, near, left, right, who, wide=512):
    tokens, width = near.shape
    rows, _ = left[0].shape
    args = [states, labels, near, *left, *right]
    far = pl.BlockSpec(memory_space=pltpu.HBM)
    powers = jax.ShapeDtypeStruct((tokens, width), BF)
    stats = jax.ShapeDtypeStruct((NY * NZ, 3, tokens), F32)
    peaks = jax.ShapeDtypeStruct((1, tokens), F32)
    count = width // wide
    return call(
        far_kernel,
        who,
        args,
        [far, whole(labels)] + [far] * 5,
        [whole(powers), whole(stats), whole(peaks)],
        [powers, stats, peaks],
        4 * tokens * rows * width,
        [
            pltpu.VMEM((tokens, width), F32),
            pltpu.VMEM((count, 2 * rows, wide), BF),
            pltpu.VMEM((tokens, 2 * rows), BF),
            pltpu.SemaphoreType.DMA((2 + 3 * count,)),
        ],
        steps=1,
        room=ROOM,
    )


def terms_kernel(starts, powers, labels, parts, peaks, *refs):
    *arrays, out, scales, losses, errors = refs
    step = pl.program_id(0)
    width, tokens = errors.shape

    @pl.when(step == 0)
    def _():
        theirs = parts[:, 0, :]
        peak = jnp.max(theirs, axis=0, keepdims=True)
        total = jnp.sum(parts[:, 1, :] * jnp.exp(theirs - peak), axis=0, keepdims=True)
        target = jnp.sum(parts[:, 2, :], axis=0, keepdims=True)
        scale = jnp.exp(peaks[...] - peak) / total
        loss = jnp.log(total) + peak - target
        scales[...] = scale
        losses[...] = loss
        columns = starts[8] + lax.broadcasted_iota(jnp.int32, (width, tokens), 0)
        hit = jnp.where(columns == labels[...], 1.0, 0.0)
        errors[...] = (powers[...].T.astype(F32) * scale - hit).astype(BF)

    half = width // 2
    own, left, right = arrays[:2], arrays[2:8], arrays[8:]
    lefts = jnp.concatenate([a[:, :half] for a in own] + [a[...] for a in left], axis=0)
    rights = jnp.concatenate([a[:, half:] for a in own] + [a[...] for a in right], axis=0)
    term = dot(lefts, errors[:half, :]) + dot(rights, errors[half:, :])
    rows = own[0].shape[0]
    for k in range(8):
        at = pl.ds(pl.multiple_of(starts[k] + step * rows, 32), rows)
        out[at, :] = term[k * rows : (k + 1) * rows].astype(BF)


def state_terms(powers, labels, parts, peaks, own, left, right, starts, depth):
    tokens, width = powers.shape
    rows = own[0].shape[0] // STEPS
    args = [powers, labels, parts, peaks, *own, *left, *right]
    specs = [whole(a) for a in args[:4]]
    specs += [pl.BlockSpec((rows, a.shape[1]), lambda j, s: (j, 0)) for a in args[4:]]
    terms = jax.ShapeDtypeStruct((depth, tokens), BF)
    line = jax.ShapeDtypeStruct((1, tokens), F32)
    return call(
        terms_kernel,
        starts,
        args,
        specs,
        [whole(terms), whole(line), whole(line)],
        [terms, line, line],
        2 * tokens * width * depth,
        [pltpu.VMEM((width, tokens), BF)],
    )


def grad_kernel(who, p0, p1, p2, p3, *refs):
    *arrays, out, states, turned = refs
    scales, arrays = arrays[:4], arrays[4:]
    step = pl.program_id(0)
    groups, padded, tokens = p0.shape
    part = padded - 16
    wide = out.shape[1]

    @pl.when(step == 0)
    def _():
        for j, parts in enumerate((p0, p1, p2, p3)):
            at = pl.multiple_of(((who[9] + j) % NY) * part, 32)
            for k in range(groups):
                states[k, pl.ds(at, part), :] = parts[k, :part, :]
        for k in range(groups):
            digits = p0[who[k], part:, :].astype(F32)
            number = digits[0:1] * 256.0 + digits[1:2]
            scale = scales[k // 2][k % 2 : k % 2 + 1, :]
            both = jnp.concatenate([number, scale, digits[:6]], axis=0)
            turned[k] = both.T

    columns = who[8] + step * wide + lax.broadcasted_iota(jnp.int32, (tokens, wide), 1)
    columns = columns.astype(F32)
    blocks = [a[...] for a in arrays]
    acc = None
    for pair in range(4):
        left, right = [], []
        for k in (2 * pair, 2 * pair + 1):
            hit = jnp.where(turned[k][:, 0:1] == columns, 1.0, 0.0)
            right.append((blocks[k].astype(F32) * turned[k][:, 1:2] - hit).astype(BF))
            left.append(states[who[k]])
        term = dot(jnp.concatenate(left, axis=1), jnp.concatenate(right, axis=0))
        acc = term if acc is None else acc + term
    out[...] = acc


def head_grad_of(parts, scales, blocks, who):
    groups, padded, tokens = parts[0].shape
    rows = NY * (padded - 16)
    width = blocks[0].shape[1]
    wide = width // STEPS
    args = [*parts, *scales, *blocks]
    specs = [whole(a) for a in args[:8]]
    specs += [pl.BlockSpec((tokens, wide), lambda j, s: (0, j))] * 8
    return call(
        grad_kernel,
        who,
        args,
        specs,
        pl.BlockSpec((rows, wide), lambda j, s: (0, j)),
        jax.ShapeDtypeStruct((rows, width), F32),
        2 * groups * tokens * rows * width,
        [pltpu.VMEM((groups, rows, tokens), BF), pltpu.VMEM((groups, tokens, 8), F32)],
    )


def step(hidden_states, head, labels):
    x, core, y = lax.axis_index("x"), lax.axis_index("core"), lax.axis_index("y")
    vocab = y * NZ + lax.axis_index("z")
    tokens, part = hidden_states.shape
    rows, width = head.shape
    half = width // 2
    depth = NY * NZ * part
    base = vocab * width

    def who(offset):
        chip = ((x + offset) % NX) * 2
        return [chip + core, chip + 1 - core]

    left_half = head[:, :half]
    right_half = head[:, half:]
    up_left = shift(left_half, "x", NX, 1)
    down_right = shift(right_half, "x", NX, -1)
    up_right = shift(right_half, "x", NX, 1)
    down_left = shift(left_half, "x", NX, -1)
    own = [head, swap(head)]
    far_left = shift(up_left, "x", NX, 1)
    far_right = shift(down_right, "x", NX, -1)
    up_left_other, down_right_other = swap(up_left), swap(down_right)
    left = [down_left, swap(down_left)]
    right = [up_right, swap(up_right)]
    away_left = [far_left, swap(far_left)]
    away_right = [far_right, swap(far_right)]

    row = from_everyone(hidden_states.T, "z", NZ)
    parts = [row] + [shift(row, "y", NY, -j) for j in (1, 2, 3)]
    digits = jnp.stack([labels // 256, labels % 256]).astype(BF)
    digits = jnp.pad(digits, ((0, 14), (0, 0)))
    states, wanted = prepared(parts, digits, y)
    wanted = lax.all_to_all(wanted, ("x", "core"), 0, 0, tiled=True)
    far_states, wanted = lax.optimization_barrier((states, wanted))

    slices = [shift(wanted, "y", NY, -j) for j in (1, 3)]
    across = shift(wanted, "y", NY, -2)
    slices = [wanted, slices[0], across, slices[1]]
    logits = logits_part(
        states,
        own,
        [up_left, up_left_other],
        [down_right, down_right_other],
        who(0) + who(3) + who(1),
    )
    logits = logits_part(states, [], left, right, who(1) + who(3), logits)
    powers, stats, peaks = far_logits(
        far_states, labels[:, None], logits, away_left, away_right, who(2) + [base]
    )

    pow_up = shift(powers, "x", NX, 1)
    pow_down = shift(powers, "x", NX, -1)
    pow_far = shift(powers, "x", NX, 2)
    pow_own = swap(powers)
    blocks = [powers, pow_own]
    for block in (pow_up, pow_down, pow_far):
        blocks += [block, swap(block)]

    parts = lax.all_to_all(stats, ("y", "z"), 0, 0, tiled=True)
    starts = [w * rows for w in who(0) + who(3) + who(1) + who(2)]
    all_left = [up_left, up_left_other, *left, *away_left]
    all_right = [*right, down_right, down_right_other, *away_right]
    terms, scale, token_loss = state_terms(
        powers, labels[None], parts, peaks, own, all_left, all_right, starts + [base], depth
    )
    token_loss = token_loss.reshape(tokens)

    arrived = lax.all_to_all(
        terms.reshape(NY * NZ, part, tokens), ("y", "z"), 0, 0, tiled=True
    )
    state_grad = arrived.astype(F32).sum(axis=0).astype(BF).T

    pair = jnp.concatenate([scale, swap(scale)])
    scales = [pair] + [shift(pair, "x", NX, s) for s in (1, -1, 2)]
    head_grad = head_grad_of(slices, scales, blocks, who(0) + who(3) + who(1) + who(2) + [base, y])
    return (token_loss, state_grad, head_grad)


def solution(mesh):
    chips = Mesh(mesh.devices.reshape(NX, 2, NY, NZ), ("x", "core", "y", "z"))
    tok, voc = ("x", "core"), ("y", "z")
    in_specs = (P(tok, voc), P(tok, voc), P(tok))
    out_specs = (P(tok), P(tok, voc), P(tok, voc))
    return jax.shard_map(step, mesh=chips, in_specs=in_specs, out_specs=out_specs, check_vma=False)
```
